32 devices in a mesh: pipe: 4 (over z), dp: 4 (over y, x), tensor: 2 (over core).
Axes of the slice: x: 2, y: 2, z: 4, core: 2. Of those that a mesh axis runs over, the one named last changes fastest.
Arguments:
- saved_inputs: bfloat16 [3, 2, 4, 512, 4096], P(None, None, 'pipe', 'dp', 'tensor'), may hold values from -6 to 6
- proj_in: bfloat16 [2, 4, 512, 4096], P(None, 'pipe', None, 'tensor'), may hold values from -0.09375 to 0.09375
- proj_out: bfloat16 [2, 4, 512, 4096], P(None, 'pipe', None, 'tensor'), may hold values from -0.25 to 0.25
- norm_gain: float32 [2, 4, 4096], P(None, 'pipe', 'tensor'), may hold values from 0.1 to 1.9
- arriving: bfloat16 [2, 4, 512, 4096], P(None, 'pipe', 'dp', 'tensor'), may hold values from -6 to 6
- logp_grad: bfloat16 [2, 512, 4096], P(None, 'dp', 'tensor'), may hold values from -6 to 6
- rewards: float32 [2, 4, 4], P(None, 'dp'), may hold values from -4 to 4
- seq_lengths: int32 [2, 4, 4], P(None, 'dp'), may hold values from 1 to 64, 128 in all within a row
- group_ids: int32 [2, 4, 4], P(None, 'dp'), may hold values from 0 to 3
Outputs:
- grad_in: float32 [2, 4, 512, 4096], P(None, 'pipe', 'dp', 'tensor')
- grad_out: float32 [2, 4, 512, 4096], P(None, 'pipe', 'dp', 'tensor')
- leaving: bfloat16 [2, 4, 512, 4096], P(None, 'pipe', 'dp', 'tensor')
The draws below stay inside these ranges and needn't reach their ends.
Inputs may be any that keep to these rules, and one draw needn't show every extreme that they name: `seq_lengths`: the 4 lengths of one microbatch on one replica sum to 128. `group_ids`: groups take sequences from several replicas and microbatches.
All inputs are finite; a program needn't handle non-finite values.
Results may differ from the reference program's by a relative error of at most 0.023.
Values may be sent and summed in bfloat16 or wider, within the bound.
A program may use at most 128 MiB of HBM per device.

```python
import math
import jax
import jax.numpy as jnp
import numpy as np
from jax import lax

D = 4096
R = 512
ROWS = 128
SEQS = 4
STEPS = 3
NEW = 2
GROUPS = 4
MOST = 64
N_PIPE = 4
N_DP = 4
N_TENSOR = 2


def set_ends(values, stream_key, smallest, top_value):
    place = [jax.random.randint(jax.random.fold_in(stream_key, axis), (), 0, length) for axis, length in enumerate(values.shape)]
    main_axis = values.shape.index(max(values.shape))
    next_to = place[:main_axis] + [(place[main_axis] + 1) % values.shape[main_axis]] + place[main_axis + 1:]
    return values.at[tuple(place)].set(smallest).at[tuple(next_to)].set(top_value)


def block_levels(own_key, shape, split, least, largest):
    gain = 1.0
    for axis_at, blocks in split:
        heights = jax.random.uniform(jax.random.fold_in(jax.random.fold_in(own_key, 6), axis_at), (blocks,), jnp.float32, least / len(split), largest / len(split))
        gain = gain * jnp.repeat(jnp.exp(heights), shape[axis_at] // blocks).reshape((-1,) + (1,) * (len(shape) - 1 - axis_at))
    return gain


def profile(number_of, total, bound, lean):
    loads = [(1 << 20) // math.isqrt(grade ** lean) + 1 for grade in range(2, number_of + 1)]
    spare, given = total - bound - (number_of - 1), [1] * (number_of - 1)
    while spare > 0:
        movable = [i for i in range(number_of - 1) if given[i] < bound]
        pool, budget = sum([loads[i] for i in movable]), spare
        for i in movable:
            extra = min(bound - given[i], max(1, budget * loads[i] // pool), spare)
            given[i] = given[i] + extra
            spare = spare - extra
    return np.array([bound] + given)


def ragged(own_key, count, total, reach, lean):
    if count == 2:
        one = jax.random.randint(own_key, (), max(1, total - reach), min(reach, total - 1) + 1)
        return jnp.stack([one, total - one])
    lengths = jnp.asarray(profile(count, total, reach, lean), jnp.int32)
    pairs = (count - 1) // 2
    source_of, sink = lengths[1:1 + 2 * pairs:2], lengths[2:2 + 2 * pairs:2]
    slack = jnp.minimum(source_of - 1, reach - sink)
    passed = jax.random.randint(jax.random.fold_in(own_key, 1), (pairs,), 0, 1 << 20) % (slack + 1)
    lengths = lengths.at[1:1 + 2 * pairs:2].set(source_of - passed).at[2:2 + 2 * pairs:2].set(sink + passed)
    return lengths[jax.random.permutation(jax.random.fold_in(own_key, 2), count)]


def normal_values(own_key, extent, spread, reach, shards=(), kind=jnp.bfloat16):
    gain = block_levels(own_key, extent, shards, -0.22, 0.18) if shards else 1.0
    entries = jax.random.normal(own_key, extent, jnp.float32) * spread * gain
    return jnp.minimum(jnp.maximum(entries, -reach), reach).astype(kind)


def setup_inputs(seed: int = 0) -> dict:
    streams_of = jax.random.split(jax.random.key(seed), 10)
    return {
        "saved_inputs": normal_values(streams_of[0], (STEPS, 2, N_PIPE, N_DP * ROWS, D), 1.0, 6.0, ((2, 4), (3, 4), (4, 2))),
        "proj_in": normal_values(streams_of[1], (2, N_PIPE, R, D), D ** -0.5, 0.09375, ((1, 4), (3, 2))),
        "proj_out": normal_values(streams_of[2], (2, N_PIPE, R, D), R ** -0.5, 0.25, ((1, 4), (3, 2))),
        "norm_gain": jnp.clip(1.0 + 0.18 * jax.random.normal(streams_of[3], (2, N_PIPE, D), jnp.float32), 0.1, 1.9),
        "arriving": normal_values(streams_of[4], (2, N_PIPE, N_DP * ROWS, D), 1.0, 6.0, ((1, 4), (2, 4), (3, 2))),
        "logp_grad": normal_values(streams_of[5], (NEW, N_DP * ROWS, D), 1.0, 6.0, ((1, 4), (2, 2))),
        "rewards": normal_values(streams_of[6], (NEW, N_DP, SEQS), 1.0, 4.0, ((1, 4),), jnp.float32),
        "seq_lengths": jax.vmap(lambda own: ragged(own, SEQS, ROWS, MOST, 2))(jax.random.split(streams_of[7], NEW * N_DP)).reshape((NEW, N_DP, SEQS)).astype(jnp.int32),
        "group_ids": set_ends(jax.random.randint(streams_of[8], (NEW, N_DP, SEQS), 0, GROUPS), jax.random.fold_in(streams_of[8], 1), 0, GROUPS - 1).astype(jnp.int32),
    }


EPS = 1e-05

def silu_slope(values):
    sigma = jax.nn.sigmoid(values)
    return sigma * (1.0 + values * (1.0 - sigma))

def round_trip(values):
    return lax.optimization_barrier(values.astype(jnp.bfloat16)).astype(jnp.float32)

def block_product(left, right):
    count = left.shape[0]
    width = right.shape[0]
    left_blocks = left.astype(jnp.float32).reshape(count, N_TENSOR, D // N_TENSOR)
    right_blocks = right.astype(jnp.float32).reshape(width, N_TENSOR, D // N_TENSOR)
    pieces = jnp.einsum('rtd,ktd->trk', left_blocks, right_blocks)
    return lax.optimization_barrier(jnp.sum(round_trip(pieces), axis=0))

def block_back(operands):
    inputs, arrive, weight_in, weight_out, gain_row = operands
    inputs_f = inputs.astype(jnp.float32)
    squares = lax.optimization_barrier(jnp.sum(inputs_f * inputs_f, axis=-1))
    inv_rms = 1.0 / jnp.sqrt(squares / D + EPS)
    gained = (inputs_f * gain_row).astype(jnp.bfloat16)
    pre_sum = block_product(gained, weight_in)
    back_sum = block_product(arrive, weight_out)
    pre_act = inv_rms[:, None] * pre_sum
    hidden = jax.nn.silu(pre_act).astype(jnp.bfloat16)
    grad_pre = back_sum * silu_slope(pre_act)
    grad_scaled = (inv_rms[:, None] * grad_pre).astype(jnp.bfloat16)
    grad_gained = jnp.dot(grad_scaled, weight_in, preferred_element_type=jnp.float32)
    radial_sum = lax.optimization_barrier(jnp.sum(grad_pre * pre_sum, axis=-1))
    out_cot = arrive.astype(jnp.float32) + gain_row * grad_gained - inputs_f * (inv_rms ** 3 * radial_sum / D)[:, None]
    return (out_cot.astype(jnp.bfloat16), grad_scaled, hidden)

def top_cotangent(logp_grad, rewards, seq_lengths, group_ids):
    groups = jnp.arange(GROUPS, dtype=jnp.int32)
    member = (group_ids[..., None] == groups).astype(jnp.float32)
    sums = lax.optimization_barrier(jnp.sum(member * rewards[..., None], axis=(0, 1, 2)))
    counts = lax.optimization_barrier(jnp.sum(member, axis=(0, 1, 2)))
    means = sums / jnp.maximum(counts, 1.0)
    advantage = rewards - lax.optimization_barrier(jnp.sum(member * means, axis=-1))
    ends = jnp.cumsum(seq_lengths, axis=-1).astype(jnp.int32)
    position = jnp.arange(ROWS, dtype=jnp.int32)
    segment = lax.optimization_barrier(jnp.sum((position[:, None] >= ends[..., None, :]).astype(jnp.int32), axis=-1))
    pick = (segment[..., None] == jnp.arange(SEQS, dtype=jnp.int32)).astype(jnp.float32)
    weights = lax.optimization_barrier(jnp.sum(pick * advantage[..., None, :], axis=-1)).reshape(NEW, N_DP * ROWS)
    return (-weights[..., None] * logp_grad.astype(jnp.float32)).astype(jnp.bfloat16)

def reference(saved_inputs, proj_in, proj_out, norm_gain, arriving, logp_grad, rewards, seq_lengths, group_ids):
    entering = top_cotangent(logp_grad, rewards, seq_lengths, group_ids)
    slots = 2 * N_PIPE
    tokens = N_DP * ROWS
    weights_in = proj_in.reshape(slots, R, D)
    weights_out = proj_out.reshape(slots, R, D)
    gains = norm_gain.reshape(slots, D)
    current = arriving
    cot_list = []
    scaled_list = []
    hidden_list = []
    out_cot = arriving
    for step_index in range(STEPS):
        inputs = saved_inputs[step_index].reshape(slots, tokens, D)
        flat_cot = current.reshape(slots, tokens, D)
        out_flat, grad_scaled, hidden = lax.map(block_back, (inputs, flat_cot, weights_in, weights_out, gains))
        cot_list.append(flat_cot)
        scaled_list.append(grad_scaled)
        hidden_list.append(hidden)
        out_cot = out_flat.reshape(2, N_PIPE, tokens, D)
        if step_index + 1 < STEPS:
            lower = jnp.concatenate([out_cot[0, 1:], out_cot[1, :1]], axis=0)
            upper = jnp.concatenate([out_cot[1, 1:], entering[step_index][None]], axis=0)
            current = jnp.stack([lower, upper])
    cot_all = jnp.stack(cot_list)
    scaled_all = jnp.stack(scaled_list)
    hidden_all = jnp.stack(hidden_list)
    saved_all = saved_inputs.reshape(STEPS, slots, tokens, D)
    scale = 1.0 / (N_DP * ROWS)

    def slot_grads(slot):
        slot = slot.astype(jnp.int32)
        inputs = lax.dynamic_index_in_dim(saved_all, slot, 1, keepdims=False)
        arrive = lax.dynamic_index_in_dim(cot_all, slot, 1, keepdims=False)
        grad_scaled = lax.dynamic_index_in_dim(scaled_all, slot, 1, keepdims=False)
        hidden = lax.dynamic_index_in_dim(hidden_all, slot, 1, keepdims=False)
        gain_row = lax.dynamic_index_in_dim(gains, slot, 0, keepdims=False)
        gained = (inputs.astype(jnp.float32) * gain_row).astype(jnp.bfloat16)
        left_in = grad_scaled.astype(jnp.float32).reshape(STEPS, N_DP, ROWS, R)
        right_in = gained.astype(jnp.float32).reshape(STEPS, N_DP, ROWS, D)
        per_in = jnp.einsum('snrk,snrd->nkd', left_in, right_in)
        left_out = hidden.astype(jnp.float32).reshape(STEPS, N_DP, ROWS, R)
        right_out = arrive.astype(jnp.float32).reshape(STEPS, N_DP, ROWS, D)
        per_out = jnp.einsum('snrk,snrd->nkd', left_out, right_out)
        total_in = lax.optimization_barrier(jnp.sum(round_trip(per_in), axis=0)) * scale
        total_out = lax.optimization_barrier(jnp.sum(round_trip(per_out), axis=0)) * scale
        return (total_in, total_out)
    grad_in, grad_out = lax.map(slot_grads, jnp.arange(slots, dtype=jnp.int32))
    return (grad_in.reshape(2, N_PIPE, R, D), grad_out.reshape(2, N_PIPE, R, D), out_cot)
```

```python
import functools

import jax
import jax.numpy as jnp
from jax import lax
from jax.experimental import pallas as pl
from jax.experimental.pallas import tpu as pltpu
from jax.sharding import PartitionSpec as P

EPS = 1e-05
MESH = pl.DeviceIdType.MESH
F32 = jnp.float32
BF16 = jnp.bfloat16


def dot_nt(a, b):
    return lax.dot_general(a, b, (((1,), (1,)), ((), ())), preferred_element_type=F32)


def dot_tn(a, b):
    return lax.dot_general(a, b, (((0,), (0,)), ((), ())), preferred_element_type=F32)


def factors(n):
    low = 1
    for k in range(1, n + 1):
        if n % k == 0 and k * k <= n:
            low = k
    return low, n // low


def kernel(
    dims,
    x_hbm, wi_hbm, wo_hbm, gn_ref, ar_hbm, lp_hbm, st_ref, hot_ref,
    gi_hbm, go_hbm, lv_hbm,
    xs, gd, ca, wi, wo, lp, ps, pr, presum, slope, hid, gs, bs, br, ob, lv,
    sqs, sqr, inv_t, str_, gbi, gbo, r1i, r1o, p2i, p2o, r2i, r2o, fi, fo,
    in_sem, out_sem, sq_sem, st_sem, pre_sem, back_sem, pipe_s, pipe_r, r1_s, r1_r, r2_s, r2_r,
):
    steps, vs, tok, wid, rank, nt, npipe, ndp = dims
    na, nb = factors(ndp)
    rc = rank // ndp
    full = wid * nt
    tile = min(256, wid)
    rtile = min(256, rank)
    me_t = lax.axis_index("tensor")
    me_p = lax.axis_index("pipe")
    me_d = lax.axis_index("dp")
    me_h = me_d // nb
    me_l = me_d % nb
    prev_p = lax.rem(me_p + npipe - 1, npipe)
    next_p = lax.rem(me_p + 1, npipe)

    def load(src, dst, k):
        return pltpu.make_async_copy(src, dst, in_sem.at[k])

    loads = [
        load(x_hbm, xs, 0),
        load(wi_hbm.at[1], wi.at[1], 1),
        load(wi_hbm.at[0], wi.at[0], 2),
        load(ar_hbm.at[1], ca.at[1, 0], 3),
        load(wo_hbm.at[1], wo.at[1], 4),
        load(ar_hbm.at[0], ca.at[0, 0], 5),
        load(wo_hbm.at[0], wo.at[0], 6),
        load(lp_hbm, lp, 7),
    ]
    for item in loads:
        item.start()

    barrier = pltpu.get_barrier_semaphore()
    for k in range(1, nt):
        pl.semaphore_signal(barrier, inc=1, device_id={"tensor": lax.rem(me_t + k, nt)}, device_id_type=MESH)
    for k in range(1, ndp):
        pl.semaphore_signal(barrier, inc=1, device_id={"dp": lax.rem(me_d + k, ndp)}, device_id_type=MESH)
    for other in (prev_p, next_p):
        pl.semaphore_signal(barrier, inc=1, device_id={"pipe": other}, device_id_type=MESH)
    pl.semaphore_wait(barrier, nt - 1 + ndp - 1 + 2)

    def to_tensor(src, dst_of, send_of, recv_of):
        return [
            pltpu.make_async_remote_copy(
                src_ref=src, dst_ref=dst_of(k - 1), send_sem=send_of(k - 1), recv_sem=recv_of(k - 1),
                device_id={"tensor": lax.rem(me_t + k, nt)}, device_id_type=MESH,
            )
            for k in range(1, nt)
        ]

    def to_dp(src_of, dst_of, send_of, recv_of, kind):
        out = []
        count = {"all": ndp, "h": na, "l": nb}[kind]
        for k in range(1, count):
            if kind == "all":
                who = lax.rem(me_d + k, ndp)
                part = who
            elif kind == "h":
                part = lax.rem(me_h + k, na)
                who = part * nb + me_l
            else:
                part = lax.rem(me_l + k, nb)
                who = me_h * nb + part
            out.append(
                pltpu.make_async_remote_copy(
                    src_ref=src_of(part), dst_ref=dst_of(k - 1), send_sem=send_of(k - 1), recv_sem=recv_of(k - 1),
                    device_id={"dp": who}, device_id_type=MESH,
                )
            )
        return out

    stat_copies = to_dp(lambda part: st_ref, lambda k: str_.at[k], lambda k: st_sem.at[0, k], lambda k: st_sem.at[1, k], "all")
    for item in stat_copies:
        item.start()

    loads[0].wait()
    lane = lax.broadcasted_iota(jnp.int32, (tok, 128), 1)
    sqs[...] = jnp.zeros_like(sqs)

    def prep(i, carry):
        t = i // vs
        v = i % vs
        row = xs[t, v].astype(F32)
        gd[v, pl.ds(pl.multiple_of(t * tok, tok), tok), :] = (row * gn_ref[v]).astype(BF16)
        squares = jnp.sum(row * row, axis=-1, keepdims=True)
        sqs[...] = jnp.where(lane == i, squares, sqs[...])
        return carry

    lax.fori_loop(0, steps * vs, prep, 0)
    sq_copies = to_tensor(sqs, lambda k: sqr.at[k], lambda k: sq_sem.at[0, k], lambda k: sq_sem.at[1, k])
    for item in sq_copies:
        item.start()

    pre_copies = {}
    back_copies = {}

    def pre_part(v):
        def body(j, carry):
            cols = pl.ds(pl.multiple_of(j * rtile, rtile), rtile)
            ps[v, :, cols] = dot_nt(gd[v], wi[v, cols, :]).astype(BF16)
            return carry

        lax.fori_loop(0, rank // rtile, body, 0)
        pre_copies[v] = to_tensor(
            ps.at[v], lambda k: pr.at[k, v], lambda k: pre_sem.at[0, v, k], lambda k: pre_sem.at[1, v, k]
        )
        for item in pre_copies[v]:
            item.start()

    def back_part(t, v):
        def body(j, carry):
            cols = pl.ds(pl.multiple_of(j * rtile, rtile), rtile)
            bs[v, t, :, cols] = dot_nt(ca[v, t], wo[v, cols, :]).astype(BF16)
            return carry

        lax.fori_loop(0, rank // rtile, body, 0)
        back_copies[t, v] = to_tensor(
            bs.at[v, t], lambda k: br.at[k, v, t],
            lambda k: back_sem.at[0, v * steps + t, k], lambda k: back_sem.at[1, v * steps + t, k],
        )
        for item in back_copies[t, v]:
            item.start()

    def finish_pre(v):
        for item in pre_copies[v]:
            item.wait_recv()
        for t in range(steps):
            rows = pl.ds(t * tok, tok)
            total = ps[v, rows, :].astype(F32)
            for k in range(nt - 1):
                total = total + pr[k, v, rows, :].astype(F32)
            index = t * vs + v
            pre = inv_t[:, index:index + 1] * total
            sigma = jax.nn.sigmoid(pre)
            presum[v, rows, :] = total
            hid[v, rows, :] = (pre * sigma).astype(BF16)
            slope[v, rows, :] = sigma * (1.0 + pre * (1.0 - sigma))

    def finish_back(t, v):
        for item in back_copies[t, v]:
            item.wait_recv()
        rows = pl.ds(t * tok, tok)
        index = t * vs + v
        inv = inv_t[:, index:index + 1]
        total = bs[v, t].astype(F32)
        for k in range(nt - 1):
            total = total + br[k, v, t].astype(F32)
        grad_pre = total * slope[v, rows, :]
        gs[v, rows, :] = (inv * grad_pre).astype(BF16)
        radial = jnp.sum(grad_pre * presum[v, rows, :], axis=-1, keepdims=True)
        coef = inv * inv * inv * radial * (1.0 / full)

        def body(j, carry):
            cols = pl.ds(pl.multiple_of(j * tile, tile), tile)
            lifted = jnp.dot(gs[v, rows, :], wi[v, :, cols], preferred_element_type=F32)
            out = (
                ca[v, t, :, cols].astype(F32)
                + gn_ref[v, :, cols] * lifted
                - xs[t, v, :, cols].astype(F32) * coef
            ).astype(BF16)
            if t < steps - 1:
                ob[t, v, :, cols] = out
            else:
                lv[v, :, cols] = out
            return carry

        lax.fori_loop(0, wid // tile, body, 0)

    def pipe_copy(t, v, slot):
        return pltpu.make_async_remote_copy(
            src_ref=ob.at[t, v], dst_ref=ca.at[slot, t + 1],
            send_sem=pipe_s.at[t, v], recv_sem=pipe_r.at[t, slot],
            device_id={"pipe": prev_p}, device_id_type=MESH,
        )

    def send_on(t, v):
        @pl.when(me_p > 0)
        def _():
            pipe_copy(t, v, v).start()

        if v == 1:
            @pl.when(me_p == 0)
            def _():
                pipe_copy(t, 1, 0).start()

    def sent_on(t, v):
        @pl.when(me_p > 0)
        def _():
            pipe_copy(t, v, v).wait_send()

        if v == 1:
            @pl.when(me_p == 0)
            def _():
                pipe_copy(t, 1, 0).wait_send()

    def take(t, v):
        if v == 0:
            pipe_copy(t - 1, v, v).wait_recv()
        else:
            @pl.when(me_p < npipe - 1)
            def _():
                pipe_copy(t - 1, v, v).wait_recv()

            @pl.when(me_p == npipe - 1)
            def _():
                stats = st_ref[...]
                for k in range(ndp - 1):
                    stats = stats + str_[k]
                means = stats[0:1] / jnp.maximum(stats[1:2], 1.0) + stats[2:3] * (1.0 / ndp)
                weight = jnp.sum(hot_ref[t - 1] * means, axis=-1, keepdims=True)
                ca[1, t] = (weight * lp[t - 1].astype(F32)).astype(BF16)

    def grad_cols(left_ref, right_of, dest, v):
        def body(j, carry):
            cols = pl.ds(pl.multiple_of(j * tile, tile), tile)
            value = dot_tn(left_ref[v], right_of(v, cols)).astype(BF16)
            dest[v, :, :, :, cols] = value.reshape(na, nb, rc, tile)
            return carry

        lax.fori_loop(0, wid // tile, body, 0)

    def copies_one(which, v):
        base = which * vs + v
        if which == 0:
            return to_dp(
                lambda part: gbi.at[v, part], lambda k: r1i.at[v, k],
                lambda k: r1_s.at[base, k], lambda k: r1_r.at[base, k], "h",
            )
        return to_dp(
            lambda part: gbo.at[v, :, part], lambda k: r1o.at[v, k],
            lambda k: r1_s.at[base, k], lambda k: r1_r.at[base, k], "l",
        )

    def copies_two(which, v):
        base = which * vs + v
        if which == 0:
            return to_dp(
                lambda part: p2i.at[v, part], lambda k: r2i.at[v, k],
                lambda k: r2_s.at[base, k], lambda k: r2_r.at[base, k], "l",
            )
        return to_dp(
            lambda part: p2o.at[v, part], lambda k: r2o.at[v, k],
            lambda k: r2_s.at[base, k], lambda k: r2_r.at[base, k], "h",
        )

    def middle(which, v):
        for item in copies_one(which, v):
            item.wait_recv()
        if which == 0:
            total = gbi[v, me_h].astype(F32)
            for k in range(na - 1):
                total = total + r1i[v, k].astype(F32)
            p2i[v] = total.astype(BF16)
        else:
            total = gbo[v, :, me_l].astype(F32)
            for k in range(nb - 1):
                total = total + r1o[v, k].astype(F32)
            p2o[v] = total.astype(BF16)
        for item in copies_two(which, v):
            item.start()

    scale = 1.0 / (ndp * tok)

    def final(which, v):
        for item in copies_two(which, v):
            item.wait_recv()
        if which == 0:
            total = p2i[v, me_l].astype(F32)
            for k in range(nb - 1):
                total = total + r2i[v, k].astype(F32)
            fi[v] = total * scale
            copy = pltpu.make_async_copy(fi.at[v], gi_hbm.at[v], out_sem.at[v])
        else:
            total = p2o[v, me_h].astype(F32)
            for k in range(na - 1):
                total = total + r2o[v, k].astype(F32)
            fo[v] = total * scale
            copy = pltpu.make_async_copy(fo.at[v], go_hbm.at[v], out_sem.at[vs + v])
        copy.start()
        return copy

    loads[1].wait()
    pre_part(1)
    loads[3].wait()
    loads[4].wait()
    back_part(0, 1)
    for item in sq_copies:
        item.wait_recv()
    total_sq = sqs[...]
    for k in range(nt - 1):
        total_sq = total_sq + sqr[k]
    inv_t[...] = 1.0 / jnp.sqrt(total_sq * (1.0 / full) + EPS)
    loads[2].wait()
    pre_part(0)
    finish_pre(1)
    finish_back(0, 1)
    send_on(0, 1)
    loads[5].wait()
    loads[6].wait()
    back_part(0, 0)
    finish_pre(0)
    finish_back(0, 0)
    send_on(0, 0)
    loads[7].wait()
    for item in stat_copies:
        item.wait_recv()
    stored = []
    for t in range(1, steps):
        for v in (1, 0):
            take(t, v)
            back_part(t, v)
            if t == steps - 1:
                grad_cols(hid, lambda u, cols: ca[u, :, :, cols].reshape(steps * tok, tile), gbo, v)
                for item in copies_one(1, v):
                    item.start()
            finish_back(t, v)
            if t < steps - 1:
                send_on(t, v)
            else:
                grad_cols(gs, lambda u, cols: gd[u, :, cols], gbi, v)
                for item in copies_one(0, v):
                    item.start()
                copy = pltpu.make_async_copy(lv.at[v], lv_hbm.at[v], out_sem.at[2 * vs + v])
                copy.start()
                stored.append(copy)
    for v in (1, 0):
        middle(1, v)
        middle(0, v)
    for v in (1, 0):
        stored.append(final(1, v))
        stored.append(final(0, v))
    for item in stat_copies + sq_copies:
        item.wait_send()
    for v in range(vs):
        for item in pre_copies[v]:
            item.wait_send()
        for t in range(steps):
            for item in back_copies[t, v]:
                item.wait_send()
            if t < steps - 1:
                sent_on(t, v)
        for which in range(2):
            for item in copies_one(which, v) + copies_two(which, v):
                item.wait_send()
    for item in stored:
        item.wait()


def shards(
    saved_inputs, proj_in, proj_out, norm_gain, arriving, logp_grad, rewards, seq_lengths, group_ids
):
    nt = lax.axis_size("tensor")
    npipe = lax.axis_size("pipe")
    ndp = lax.axis_size("dp")
    steps, vs, _, tok, wid = saved_inputs.shape
    rank = proj_in.shape[2]
    new_count = logp_grad.shape[0]
    seq_count = rewards.shape[2]
    group_count = new_count * ndp * seq_count // 8
    lanes = -(-(group_count + 1) // 128) * 128
    na, nb = factors(ndp)
    rc = rank // ndp

    groups = jnp.arange(lanes, dtype=jnp.int32)
    member = (group_ids[..., None] == groups).astype(F32)
    sums = jnp.sum(member * rewards[..., None], axis=(0, 1, 2))
    counts = jnp.sum(member, axis=(0, 1, 2))
    unit = (groups == group_count).astype(F32)
    blank = jnp.zeros_like(unit)
    stats = jnp.stack([sums, counts, unit, blank, blank, blank, blank, blank])
    ends = jnp.cumsum(seq_lengths[:, 0], axis=-1)
    position = jnp.arange(tok, dtype=jnp.int32)
    starts = ends - seq_lengths[:, 0]
    pick = (position[:, None] >= starts[:, None, :]) & (position[:, None] < ends[:, None, :])
    seq_rows = member[:, 0] - unit * rewards[:, 0, :, None]
    hot = jnp.sum(jnp.where(pick[..., None], seq_rows[:, None], 0.0), axis=2)

    dims = (steps, vs, tok, wid, rank, nt, npipe, ndp)
    peers = max(nt - 1, 1)
    any_spec = pl.BlockSpec(memory_space=pl.ANY)
    vmem = pl.BlockSpec(memory_space=pltpu.VMEM)
    V = pltpu.VMEM
    DMA = pltpu.SemaphoreType.DMA
    pmax = max(na, nb)
    scratch = [
        V((steps, vs, tok, wid), BF16),
        V((vs, steps * tok, wid), BF16),
        V((vs, steps, tok, wid), BF16),
        V((vs, rank, wid), BF16),
        V((vs, rank, wid), BF16),
        V((new_count, tok, wid), BF16),
        V((vs, steps * tok, rank), BF16),
        V((peers, vs, steps * tok, rank), BF16),
        V((vs, steps * tok, rank), F32),
        V((vs, steps * tok, rank), F32),
        V((vs, steps * tok, rank), BF16),
        V((vs, steps * tok, rank), BF16),
        V((vs, steps, tok, rank), BF16),
        V((peers, vs, steps, tok, rank), BF16),
        V((steps - 1, vs, tok, wid), BF16),
        V((vs, tok, wid), BF16),
        V((tok, 128), F32),
        V((peers, tok, 128), F32),
        V((tok, 128), F32),
        V((max(ndp - 1, 1), 8, lanes), F32),
        V((vs, na, nb, rc, wid), BF16),
        V((vs, na, nb, rc, wid), BF16),
        V((vs, max(na - 1, 1), nb, rc, wid), BF16),
        V((vs, max(nb - 1, 1), na, rc, wid), BF16),
        V((vs, nb, rc, wid), BF16),
        V((vs, na, rc, wid), BF16),
        V((vs, max(nb - 1, 1), rc, wid), BF16),
        V((vs, max(na - 1, 1), rc, wid), BF16),
        V((vs, rc, wid), F32),
        V((vs, rc, wid), F32),
        DMA((8,)),
        DMA((3 * vs,)),
        DMA((2, peers)),
        DMA((2, max(ndp - 1, 1))),
        DMA((2, vs, peers)),
        DMA((2, vs * steps, peers)),
        DMA((steps - 1, vs)),
        DMA((steps - 1, vs)),
        DMA((2 * vs, pmax)),
        DMA((2 * vs, pmax)),
        DMA((2 * vs, pmax)),
        DMA((2 * vs, pmax)),
    ]
    grad_in, grad_out, leaving = pl.pallas_call(
        functools.partial(kernel, dims),
        out_shape=(
            jax.ShapeDtypeStruct((vs, rc, wid), F32),
            jax.ShapeDtypeStruct((vs, rc, wid), F32),
            jax.ShapeDtypeStruct((vs, tok, wid), BF16),
        ),
        in_specs=[any_spec, any_spec, any_spec, vmem, any_spec, any_spec, vmem, vmem],
        out_specs=(any_spec, any_spec, any_spec),
        scratch_shapes=scratch,
        compiler_params=pltpu.CompilerParams(
            collective_id=0, has_side_effects=True, vmem_limit_bytes=67043328
        ),
    )(
        saved_inputs[:, :, 0], proj_in[:, 0], proj_out[:, 0], norm_gain, arriving[:, 0], logp_grad, stats, hot
    )
    return grad_in[:, None], grad_out[:, None], leaving[:, None]


def solution(mesh):
    return jax.shard_map(
        shards,
        mesh=mesh,
        in_specs=(
            P(None, None, "pipe", "dp", "tensor"),
            P(None, "pipe", None, "tensor"),
            P(None, "pipe", None, "tensor"),
            P(None, "pipe", "tensor"),
            P(None, "pipe", "dp", "tensor"),
            P(None, "dp", "tensor"),
            P(None, "dp", None),
            P(None, "dp", None),
            P(None, "dp", None),
        ),
        out_specs=(
            P(None, "pipe", "dp", "tensor"),
            P(None, "pipe", "dp", "tensor"),
            P(None, "pipe", "dp", "tensor"),
        ),
        check_vma=False,
    )
```

```python
import functools

import jax
import jax.numpy as jnp
from jax import lax
from jax.experimental import pallas as pl
from jax.experimental.pallas import tpu as pltpu
from jax.sharding import PartitionSpec as P

EPS = 1e-05
MESH = pl.DeviceIdType.MESH
F32 = jnp.float32
BF16 = jnp.bfloat16


def dot_nt(a, b):
    return lax.dot_general(a, b, (((1,), (1,)), ((), ())), preferred_element_type=F32)


def factors(n):
    low = 1
    for k in range(1, n + 1):
        if n % k == 0 and k * k <= n:
            low = k
    return low, n // low


def kernel(
    dims,
    x_hbm, wi_hbm, wo_hbm, gn_ref, ar_hbm, lp_hbm, rew_ref, len_ref, ids_ref,
    fi, fo, lv,
    xs, gd, ca, wi, wo, lp, ps, pr, presum, slope, hid_t, gs, gs_t, gsr0, gsr1, gdr0, gdr1, bs, br, ob,
    sqs, sqr, inv_t, stl, str_, gba, gbb, r1a, r1b, p2a, p2b, r2a, r2b, p2i0, p2i1, r2i0, r2i1,
    in_sem, sq_sem, st_sem, pre_sem, back_sem, pipe_s, pipe_r, gd_s, gd_r, gt_s, gt_r,
    r1_s, r1_r, r2_s, r2_r,
):
    steps, vs, tok, wid, rank, nt, npipe, ndp = dims
    na, nb = factors(ndp)
    rc = rank // ndp
    full = wid * nt
    tile = min(256, wid)
    rtile = min(256, rank)
    half = wid // 2
    lanes = stl.shape[1]
    new_count, _, seq_count = rew_ref.shape
    unit_lane = new_count * ndp * seq_count // 8
    me_t = lax.axis_index("tensor")
    me_p = lax.axis_index("pipe")
    me_d = lax.axis_index("dp")
    me_h = me_d // nb
    me_l = me_d % nb
    prev_p = lax.rem(me_p + npipe - 1, npipe)
    next_p = lax.rem(me_p + 1, npipe)

    def load(src, dst, k):
        return pltpu.make_async_copy(src, dst, in_sem.at[k])

    loads = [
        load(x_hbm, xs, 0),
        load(wi_hbm.at[1], wi.at[1], 1),
        load(wi_hbm.at[0], wi.at[0], 2),
        load(ar_hbm.at[1], ca.at[1, 0], 3),
        load(wo_hbm.at[1], wo.at[1], 4),
        load(ar_hbm.at[0], ca.at[0, 0], 5),
        load(wo_hbm.at[0], wo.at[0], 6),
        load(lp_hbm, lp, 7),
    ]
    for item in loads:
        item.start()

    lane8 = lax.broadcasted_iota(jnp.int32, (8, lanes), 1)
    row8 = lax.broadcasted_iota(jnp.int32, (8, lanes), 0)
    stats_own = jnp.where((row8 == 2) & (lane8 == unit_lane), 1.0, 0.0)
    for n in range(new_count):
        for k in range(seq_count):
            value = jnp.where(row8 == 0, rew_ref[n, 0, k], jnp.where(row8 == 1, 1.0, 0.0))
            stats_own = stats_own + jnp.where(lane8 == ids_ref[n, 0, k], value, 0.0)
    stl[...] = stats_own

    barrier = pltpu.get_barrier_semaphore()
    for k in range(1, nt):
        pl.semaphore_signal(barrier, inc=1, device_id={"tensor": lax.rem(me_t + k, nt)}, device_id_type=MESH)
    for k in range(1, ndp):
        pl.semaphore_signal(barrier, inc=1, device_id={"dp": lax.rem(me_d + k, ndp)}, device_id_type=MESH)
    for other in (prev_p, next_p):
        pl.semaphore_signal(barrier, inc=1, device_id={"pipe": other}, device_id_type=MESH)
    pl.semaphore_wait(barrier, nt - 1 + ndp - 1 + 2)

    def to_tensor(src, dst_of, send_of, recv_of):
        return [
            pltpu.make_async_remote_copy(
                src_ref=src, dst_ref=dst_of(k - 1), send_sem=send_of(k - 1), recv_sem=recv_of(k - 1),
                device_id={"tensor": lax.rem(me_t + k, nt)}, device_id_type=MESH,
            )
            for k in range(1, nt)
        ]

    def to_dp(src_of, dst_of, send_of, recv_of, kind):
        out = []
        count = {"all": ndp, "h": na, "l": nb}[kind]
        for k in range(1, count):
            if kind == "all":
                who = lax.rem(me_d + k, ndp)
                part = who
            elif kind == "h":
                part = lax.rem(me_h + k, na)
                who = part * nb + me_l
            else:
                part = lax.rem(me_l + k, nb)
                who = me_h * nb + part
            out.append(
                pltpu.make_async_remote_copy(
                    src_ref=src_of(part), dst_ref=dst_of(k - 1), send_sem=send_of(k - 1), recv_sem=recv_of(k - 1),
                    device_id={"dp": who}, device_id_type=MESH,
                )
            )
        return out

    stat_copies = to_dp(lambda part: stl, lambda k: str_.at[k], lambda k: st_sem.at[0, k], lambda k: st_sem.at[1, k], "all")
    for item in stat_copies:
        item.start()

    loads[0].wait()
    lane = lax.broadcasted_iota(jnp.int32, (tok, 128), 1)
    sqs[...] = jnp.zeros_like(sqs)

    def prep(i, carry):
        t = i // vs
        v = i % vs
        row = xs[t, v].astype(F32)
        gd[v, pl.ds(pl.multiple_of(t * tok, tok), tok), :] = (row * gn_ref[v]).astype(BF16)
        squares = jnp.sum(row * row, axis=-1, keepdims=True)
        sqs[...] = jnp.where(lane == i, squares, sqs[...])
        return carry

    lax.fori_loop(0, steps * vs, prep, 0)
    sq_copies = to_tensor(sqs, lambda k: sqr.at[k], lambda k: sq_sem.at[0, k], lambda k: sq_sem.at[1, k])
    for item in sq_copies:
        item.start()

    gather_kind = ("h", "l")
    gdr = (gdr0, gdr1)
    gsr = (gsr0, gsr1)

    def gd_copies(v):
        return to_dp(
            lambda part: gd.at[v], lambda k: gdr[v].at[k],
            lambda k: gd_s.at[v, k], lambda k: gd_r.at[v, k], gather_kind[v],
        )

    def gs_copies(t, v):
        cols = pl.ds(t * tok, tok)
        base = v * steps + t
        source = (lambda part: gs_t.at[v, part, :, :, cols]) if v == 0 else (lambda part: gs_t.at[v, :, part, :, cols])
        return to_dp(
            source, lambda k: gsr[v].at[k, :, :, cols],
            lambda k: gt_s.at[base, k], lambda k: gt_r.at[base, k], gather_kind[v],
        )

    for v in (1, 0):
        for item in gd_copies(v):
            item.start()

    pre_copies = {}
    back_copies = {}

    def pre_part(v):
        def body(j, carry):
            cols = pl.ds(pl.multiple_of(j * rtile, rtile), rtile)
            ps[v, :, cols] = dot_nt(gd[v], wi[v, cols, :]).astype(BF16)
            return carry

        lax.fori_loop(0, rank // rtile, body, 0)
        pre_copies[v] = to_tensor(
            ps.at[v], lambda k: pr.at[k, v], lambda k: pre_sem.at[0, v, k], lambda k: pre_sem.at[1, v, k]
        )
        for item in pre_copies[v]:
            item.start()

    def back_part(t, v):
        def body(j, carry):
            cols = pl.ds(pl.multiple_of(j * rtile, rtile), rtile)
            bs[v, t, :, cols] = dot_nt(ca[v, t], wo[v, cols, :]).astype(BF16)
            return carry

        lax.fori_loop(0, rank // rtile, body, 0)
        back_copies[t, v] = to_tensor(
            bs.at[v, t], lambda k: br.at[k, v, t],
            lambda k: back_sem.at[0, v * steps + t, k], lambda k: back_sem.at[1, v * steps + t, k],
        )
        for item in back_copies[t, v]:
            item.start()

    def finish_pre(v):
        for item in pre_copies[v]:
            item.wait_recv()
        for t in range(steps):
            rows = pl.ds(t * tok, tok)
            total = ps[v, rows, :].astype(F32)
            for k in range(nt - 1):
                total = total + pr[k, v, rows, :].astype(F32)
            index = t * vs + v
            pre = inv_t[:, index:index + 1] * total
            sigma = jax.nn.sigmoid(pre)
            presum[v, rows, :] = total
            hid_t[v, :, rows] = jnp.transpose(pre * sigma).astype(BF16)
            slope[v, rows, :] = sigma * (1.0 + pre * (1.0 - sigma))

    def finish_back(t, v):
        for item in back_copies[t, v]:
            item.wait_recv()
        rows = pl.ds(t * tok, tok)
        index = t * vs + v
        inv = inv_t[:, index:index + 1]
        total = bs[v, t].astype(F32)
        for k in range(nt - 1):
            total = total + br[k, v, t].astype(F32)
        grad_pre = total * slope[v, rows, :]
        scaled = inv * grad_pre
        gs[v, rows, :] = scaled.astype(BF16)
        gs_t[v, :, :, :, rows] = jnp.transpose(scaled).astype(BF16).reshape(na, nb, rc, tok)
        for item in gs_copies(t, v):
            item.start()
        if t == steps - 1:
            for item in copies_one(0, v) + copies_one(1, v):
                item.start()
        radial = jnp.sum(grad_pre * presum[v, rows, :], axis=-1, keepdims=True)
        coef = inv * inv * inv * radial * (1.0 / full)

        def body(j, carry):
            cols = pl.ds(pl.multiple_of(j * tile, tile), tile)
            lifted = jnp.dot(gs[v, rows, :], wi[v, :, cols], preferred_element_type=F32)
            out = (
                ca[v, t, :, cols].astype(F32)
                + gn_ref[v, :, cols] * lifted
                - xs[t, v, :, cols].astype(F32) * coef
            ).astype(BF16)
            if t < steps - 1:
                ob[t, v, :, cols] = out
            else:
                lv[v, :, cols] = out
            return carry

        lax.fori_loop(0, wid // tile, body, 0)

    def pipe_copy(t, v, slot):
        return pltpu.make_async_remote_copy(
            src_ref=ob.at[t, v], dst_ref=ca.at[slot, t + 1],
            send_sem=pipe_s.at[t, v], recv_sem=pipe_r.at[t, slot],
            device_id={"pipe": prev_p}, device_id_type=MESH,
        )

    def send_on(t, v):
        @pl.when(me_p > 0)
        def _():
            pipe_copy(t, v, v).start()

        if v == 1:
            @pl.when(me_p == 0)
            def _():
                pipe_copy(t, 1, 0).start()

    def sent_on(t, v):
        @pl.when(me_p > 0)
        def _():
            pipe_copy(t, v, v).wait_send()

        if v == 1:
            @pl.when(me_p == 0)
            def _():
                pipe_copy(t, 1, 0).wait_send()

    def take(t, v):
        if v == 0:
            pipe_copy(t - 1, v, v).wait_recv()
        else:
            @pl.when(me_p < npipe - 1)
            def _():
                pipe_copy(t - 1, v, v).wait_recv()

            @pl.when(me_p == npipe - 1)
            def _():
                stats = stl[...]
                for k in range(ndp - 1):
                    stats = stats + str_[k]
                means = stats[0:1] / jnp.maximum(stats[1:2], 1.0) + stats[2:3] * (1.0 / ndp)
                tok_row = lax.broadcasted_iota(jnp.int32, (tok, lanes), 0)
                tok_lane = lax.broadcasted_iota(jnp.int32, (tok, lanes), 1)
                hot = jnp.zeros((tok, lanes), F32)
                begin = 0
                for k in range(seq_count):
                    finish = begin + len_ref[t - 1, 0, k]
                    inside = (tok_row >= begin) & (tok_row < finish)
                    value = jnp.where(tok_lane == ids_ref[t - 1, 0, k], 1.0, 0.0)
                    value = value - jnp.where(tok_lane == unit_lane, rew_ref[t - 1, 0, k], 0.0)
                    hot = hot + jnp.where(inside, value, 0.0)
                    begin = finish
                weight = jnp.sum(hot * means, axis=-1, keepdims=True)
                ca[1, t] = (weight * lp[t - 1].astype(F32)).astype(BF16)

    def grad_out(v):
        def body(j, carry):
            for dest, off in ((gba, 0), (gbb, half)):
                cols = pl.ds(pl.multiple_of(j * tile, tile), tile)
                from_cols = pl.ds(pl.multiple_of(off + j * tile, tile), tile)
                right = ca[v, :, :, from_cols].reshape(steps * tok, tile)
                value = jnp.dot(hid_t[v], right, preferred_element_type=F32).astype(BF16)
                dest[v, :, :, :, cols] = value.reshape(na, nb, rc, tile)
            return carry

        lax.fori_loop(0, half // tile, body, 0)

    def grad_in(v):
        for item in gd_copies(v):
            item.wait_recv()
        for t in range(steps):
            for item in gs_copies(t, v):
                item.wait_recv()
        own = gs_t[v, me_h] if v == 0 else gs_t[v, :, me_l]
        width = nb if v == 0 else na
        own = own.reshape(width * rc, steps * tok)
        dest = p2i0 if v == 0 else p2i1

        def body(j, carry):
            cols = pl.ds(pl.multiple_of(j * tile, tile), tile)
            value = jnp.dot(own, gd[v, :, cols], preferred_element_type=F32)
            for k in range((na if v == 0 else nb) - 1):
                left = gsr[v][k].reshape(width * rc, steps * tok)
                value = value + jnp.dot(left, gdr[v][k, :, cols], preferred_element_type=F32)
            dest[:, :, cols] = value.astype(BF16).reshape(width, rc, tile)
            return carry

        lax.fori_loop(0, wid // tile, body, 0)
        for item in copies_two(2, v):
            item.start()

    def copies_one(which, v):
        base = which * vs + v
        if which == 0:
            return to_dp(
                lambda part: gba.at[v, :, part], lambda k: r1a.at[v, k],
                lambda k: r1_s.at[base, k], lambda k: r1_r.at[base, k], "l",
            )
        return to_dp(
            lambda part: gbb.at[v, part], lambda k: r1b.at[v, k],
            lambda k: r1_s.at[base, k], lambda k: r1_r.at[base, k], "h",
        )

    def copies_two(which, v):
        base = which * vs + v
        if which == 0:
            source, dest, kind = p2a.at[v], r2a.at[v], "h"
        elif which == 1:
            source, dest, kind = p2b.at[v], r2b.at[v], "l"
        elif v == 1:
            source, dest, kind = p2i1, r2i1, "h"
        else:
            source, dest, kind = p2i0, r2i0, "l"
        return to_dp(
            lambda part: source.at[part], lambda k: dest.at[k],
            lambda k: r2_s.at[base, k], lambda k: r2_r.at[base, k], kind,
        )

    def middle(which, v):
        for item in copies_one(which, v):
            item.wait_recv()
        if which == 0:
            total = gba[v, :, me_l].astype(F32)
            for k in range(nb - 1):
                total = total + r1a[v, k].astype(F32)
            p2a[v] = total.astype(BF16)
        else:
            total = gbb[v, me_h].astype(F32)
            for k in range(na - 1):
                total = total + r1b[v, k].astype(F32)
            p2b[v] = total.astype(BF16)
        for item in copies_two(which, v):
            item.start()

    scale = 1.0 / (ndp * tok)

    def final(which, v):
        for item in copies_two(which, v):
            item.wait_recv()
        along_h = which == 0 or (which == 2 and v == 1)
        source = {0: p2a.at[v], 1: p2b.at[v], 2: p2i1 if v == 1 else p2i0}[which]
        got = {0: r2a.at[v], 1: r2b.at[v], 2: r2i1 if v == 1 else r2i0}[which]
        total = source[me_h if along_h else me_l].astype(F32)
        for k in range((na if along_h else nb) - 1):
            total = total + got[k].astype(F32)
        if which == 2:
            fi[v] = total * scale
        else:
            fo[v, :, pl.ds(which * half, half)] = total * scale

    loads[1].wait()
    pre_part(1)
    loads[3].wait()
    loads[4].wait()
    back_part(0, 1)
    for item in sq_copies:
        item.wait_recv()
    total_sq = sqs[...]
    for k in range(nt - 1):
        total_sq = total_sq + sqr[k]
    inv_t[...] = 1.0 / jnp.sqrt(total_sq * (1.0 / full) + EPS)
    loads[2].wait()
    pre_part(0)
    finish_pre(1)
    finish_back(0, 1)
    send_on(0, 1)
    loads[5].wait()
    loads[6].wait()
    back_part(0, 0)
    finish_pre(0)
    finish_back(0, 0)
    send_on(0, 0)
    loads[7].wait()
    for item in stat_copies:
        item.wait_recv()
    for t in range(1, steps):
        for v in (1, 0):
            take(t, v)
            back_part(t, v)
            if t == steps - 1:
                grad_out(v)
            finish_back(t, v)
            if t < steps - 1:
                send_on(t, v)
            elif v == 1:
                grad_in(1)
    middle(0, 1)
    middle(1, 1)
    grad_in(0)
    middle(0, 0)
    middle(1, 0)
    for v in (1, 0):
        for which in (2, 0, 1):
            final(which, v)
    for item in stat_copies + sq_copies:
        item.wait_send()
    for v in range(vs):
        for item in pre_copies[v] + gd_copies(v):
            item.wait_send()
        for t in range(steps):
            for item in back_copies[t, v] + gs_copies(t, v):
                item.wait_send()
            if t < steps - 1:
                sent_on(t, v)
        for item in copies_one(0, v) + copies_one(1, v):
            item.wait_send()
        for which in range(3):
            for item in copies_two(which, v):
                item.wait_send()


def shards(
    saved_inputs, proj_in, proj_out, norm_gain, arriving, logp_grad, rewards, seq_lengths, group_ids
):
    nt = lax.axis_size("tensor")
    npipe = lax.axis_size("pipe")
    ndp = lax.axis_size("dp")
    steps, vs, _, tok, wid = saved_inputs.shape
    rank = proj_in.shape[2]
    new_count = logp_grad.shape[0]
    group_count = new_count * ndp * rewards.shape[2] // 8
    lanes = -(-(group_count + 1) // 128) * 128
    na, nb = factors(ndp)
    rc = rank // ndp
    half = wid // 2
    hm, lm = max(na - 1, 1), max(nb - 1, 1)
    dims = (steps, vs, tok, wid, rank, nt, npipe, ndp)
    peers = max(nt - 1, 1)
    any_spec = pl.BlockSpec(memory_space=pl.ANY)
    vmem = pl.BlockSpec(memory_space=pltpu.VMEM)
    V = pltpu.VMEM
    DMA = pltpu.SemaphoreType.DMA
    pmax = max(na, nb)
    smem = pl.BlockSpec(memory_space=pltpu.SMEM)
    scratch = [
        V((steps, vs, tok, wid), BF16),
        V((vs, steps * tok, wid), BF16),
        V((vs, steps, tok, wid), BF16),
        V((vs, rank, wid), BF16),
        V((vs, rank, wid), BF16),
        V((new_count, tok, wid), BF16),
        V((vs, steps * tok, rank), BF16),
        V((peers, vs, steps * tok, rank), BF16),
        V((vs, steps * tok, rank), F32),
        V((vs, steps * tok, rank), F32),
        V((vs, rank, steps * tok), BF16),
        V((vs, steps * tok, rank), BF16),
        V((vs, na, nb, rc, steps * tok), BF16),
        V((hm, nb, rc, steps * tok), BF16),
        V((lm, na, rc, steps * tok), BF16),
        V((hm, steps * tok, wid), BF16),
        V((lm, steps * tok, wid), BF16),
        V((vs, steps, tok, rank), BF16),
        V((peers, vs, steps, tok, rank), BF16),
        V((steps - 1, vs, tok, wid), BF16),
        V((tok, 128), F32),
        V((peers, tok, 128), F32),
        V((tok, 128), F32),
        V((8, lanes), F32),
        V((max(ndp - 1, 1), 8, lanes), F32),
        V((vs, na, nb, rc, half), BF16),
        V((vs, na, nb, rc, half), BF16),
        V((vs, lm, na, rc, half), BF16),
        V((vs, hm, nb, rc, half), BF16),
        V((vs, na, rc, half), BF16),
        V((vs, nb, rc, half), BF16),
        V((vs, hm, rc, half), BF16),
        V((vs, lm, rc, half), BF16),
        V((nb, rc, wid), BF16),
        V((na, rc, wid), BF16),
        V((lm, rc, wid), BF16),
        V((hm, rc, wid), BF16),
        DMA((8,)),
        DMA((2, peers)),
        DMA((2, max(ndp - 1, 1))),
        DMA((2, vs, peers)),
        DMA((2, vs * steps, peers)),
        DMA((steps - 1, vs)),
        DMA((steps - 1, vs)),
        DMA((vs, pmax)),
        DMA((vs, pmax)),
        DMA((vs * steps, pmax)),
        DMA((vs * steps, pmax)),
        DMA((2 * vs, pmax)),
        DMA((2 * vs, pmax)),
        DMA((3 * vs, pmax)),
        DMA((3 * vs, pmax)),
    ]
    grad_in, grad_out, leaving = pl.pallas_call(
        functools.partial(kernel, dims),
        out_shape=(
            V((vs, rc, wid), F32),
            V((vs, rc, wid), F32),
            V((vs, tok, wid), BF16),
        ),
        in_specs=[any_spec, any_spec, any_spec, vmem, any_spec, any_spec, smem, smem, smem],
        out_specs=(vmem, vmem, vmem),
        scratch_shapes=scratch,
        compiler_params=pltpu.CompilerParams(
            collective_id=0, has_side_effects=True, vmem_limit_bytes=56 * 1024 * 1024
        ),
    )(
        saved_inputs[:, :, 0], proj_in[:, 0], proj_out[:, 0], norm_gain, arriving[:, 0], logp_grad,
        rewards, seq_lengths, group_ids,
    )
    return grad_in[:, None], grad_out[:, None], leaving[:, None]


def solution(mesh):
    return jax.shard_map(
        shards,
        mesh=mesh,
        in_specs=(
            P(None, None, "pipe", "dp", "tensor"),
            P(None, "pipe", None, "tensor"),
            P(None, "pipe", None, "tensor"),
            P(None, "pipe", "tensor"),
            P(None, "pipe", "dp", "tensor"),
            P(None, "dp", "tensor"),
            P(None, "dp", None),
            P(None, "dp", None),
            P(None, "dp", None),
        ),
        out_specs=(
            P(None, "pipe", "dp", "tensor"),
            P(None, "pipe", "dp", "tensor"),
            P(None, "pipe", "dp", "tensor"),
        ),
        check_vma=False,
    )
```

```python
import functools

import jax
import jax.numpy as jnp
from jax import lax
from jax.experimental import pallas as pl
from jax.experimental.pallas import tpu as pltpu
from jax.sharding import PartitionSpec as P

EPS = 1e-05
MESH = pl.DeviceIdType.MESH
F32 = jnp.float32
BF16 = jnp.bfloat16


def dot_nt(a, b):
    return lax.dot_general(a, b, (((1,), (1,)), ((), ())), preferred_element_type=F32)


def factors(n):
    low = 1
    for k in range(1, n + 1):
        if n % k == 0 and k * k <= n:
            low = k
    return low, n // low


def kernel(
    dims,
    x_hbm, wi_hbm, wo_hbm, gn_ref, ar_hbm, lp_hbm, rew_ref, len_ref, ids_ref,
    fi, fo, lv,
    xs, gd, ca, wi, wo, lp, ps, pr, presum, slope, hid_t, gs, gs_t, gsr0, gsr1, gdr0, gdr1, bs, br, ob,
    sqs, sqr, inv_t, stl, str_, gba, gbb, r1a, r1b, p2a, p2b, r2a, r2b, p2i0, p2i1, r2i0, r2i1,
    in_sem, sq_sem, st_sem, pre_sem, back_sem, pipe_s, pipe_r, gd_s, gd_r, gt_s, gt_r,
    r1_s, r1_r, r2_s, r2_r,
):
    steps, vs, tok, wid, rank, nt, npipe, ndp = dims
    na, nb = factors(ndp)
    rc = rank // ndp
    full = wid * nt
    tile = min(256, wid)
    rtile = min(256, rank)
    half = wid // 2
    lanes = stl.shape[1]
    new_count, _, seq_count = rew_ref.shape
    unit_lane = new_count * ndp * seq_count // 8
    me_t = lax.axis_index("tensor")
    me_p = lax.axis_index("pipe")
    me_d = lax.axis_index("dp")
    me_h = me_d // nb
    me_l = me_d % nb
    prev_p = lax.rem(me_p + npipe - 1, npipe)
    next_p = lax.rem(me_p + 1, npipe)

    def load(src, dst, k):
        return pltpu.make_async_copy(src, dst, in_sem.at[k])

    loads = [
        load(ar_hbm.at[1], ca.at[1, 0], 0),
        load(wo_hbm.at[1], wo.at[1], 1),
        load(x_hbm.at[:, 1], xs.at[:, 1], 2),
        load(wi_hbm.at[1], wi.at[1], 3),
        load(x_hbm.at[:, 0], xs.at[:, 0], 4),
        load(ar_hbm.at[0], ca.at[0, 0], 5),
        load(wo_hbm.at[0], wo.at[0], 6),
        load(wi_hbm.at[0], wi.at[0], 7),
        load(lp_hbm, lp, 8),
    ]
    for item in loads:
        item.start()

    lane8 = lax.broadcasted_iota(jnp.int32, (8, lanes), 1)
    row8 = lax.broadcasted_iota(jnp.int32, (8, lanes), 0)
    stats_own = jnp.where((row8 == 2) & (lane8 == unit_lane), 1.0, 0.0)
    for n in range(new_count):
        for k in range(seq_count):
            value = jnp.where(row8 == 0, rew_ref[n, 0, k], jnp.where(row8 == 1, 1.0, 0.0))
            stats_own = stats_own + jnp.where(lane8 == ids_ref[n, 0, k], value, 0.0)
    stl[...] = stats_own

    barrier = pltpu.get_barrier_semaphore()
    for k in range(1, nt):
        pl.semaphore_signal(barrier, inc=1, device_id={"tensor": lax.rem(me_t + k, nt)}, device_id_type=MESH)
    for k in range(1, ndp):
        pl.semaphore_signal(barrier, inc=1, device_id={"dp": lax.rem(me_d + k, ndp)}, device_id_type=MESH)
    for other in (prev_p, next_p):
        pl.semaphore_signal(barrier, inc=1, device_id={"pipe": other}, device_id_type=MESH)
    pl.semaphore_wait(barrier, nt - 1 + ndp - 1 + 2)

    def to_tensor(src, dst_of, send_of, recv_of):
        return [
            pltpu.make_async_remote_copy(
                src_ref=src, dst_ref=dst_of(k - 1), send_sem=send_of(k - 1), recv_sem=recv_of(k - 1),
                device_id={"tensor": lax.rem(me_t + k, nt)}, device_id_type=MESH,
            )
            for k in range(1, nt)
        ]

    def to_dp(src_of, dst_of, send_of, recv_of, kind):
        out = []
        count = {"all": ndp, "h": na, "l": nb}[kind]
        for k in range(1, count):
            if kind == "all":
                who = lax.rem(me_d + k, ndp)
                part = who
            elif kind == "h":
                part = lax.rem(me_h + k, na)
                who = part * nb + me_l
            else:
                part = lax.rem(me_l + k, nb)
                who = me_h * nb + part
            out.append(
                pltpu.make_async_remote_copy(
                    src_ref=src_of(part), dst_ref=dst_of(k - 1), send_sem=send_of(k - 1), recv_sem=recv_of(k - 1),
                    device_id={"dp": who}, device_id_type=MESH,
                )
            )
        return out

    stat_copies = to_dp(lambda part: stl, lambda k: str_.at[k], lambda k: st_sem.at[0, k], lambda k: st_sem.at[1, k], "all")
    for item in stat_copies:
        item.start()

    lane = lax.broadcasted_iota(jnp.int32, (tok, 128), 1)

    def sq_copies(v):
        return to_tensor(
            sqs.at[v], lambda k: sqr.at[k, v], lambda k: sq_sem.at[0, v, k], lambda k: sq_sem.at[1, v, k]
        )

    def prep(v):
        def body(t, squares_all):
            row = xs[t, v].astype(F32)
            gd[v, pl.ds(pl.multiple_of(t * tok, tok), tok), :] = (row * gn_ref[v]).astype(BF16)
            squares = jnp.sum(row * row, axis=-1, keepdims=True)
            return jnp.where(lane == t, squares, squares_all)

        sqs[v] = lax.fori_loop(0, steps, body, jnp.zeros((tok, 128), F32))
        for item in sq_copies(v) + gd_copies(v):
            item.start()

    def finish_sq(v):
        for item in sq_copies(v):
            item.wait_recv()
        total = sqs[v]
        for k in range(nt - 1):
            total = total + sqr[k, v]
        inv_t[v] = 1.0 / jnp.sqrt(total * (1.0 / full) + EPS)

    gather_kind = ("h", "l")
    gdr = (gdr0, gdr1)
    gsr = (gsr0, gsr1)

    def gd_copies(v):
        return to_dp(
            lambda part: gd.at[v], lambda k: gdr[v].at[k],
            lambda k: gd_s.at[v, k], lambda k: gd_r.at[v, k], gather_kind[v],
        )

    def gs_copies(t, v):
        cols = pl.ds(t * tok, tok)
        base = v * steps + t
        source = (lambda part: gs_t.at[v, part, :, :, cols]) if v == 0 else (lambda part: gs_t.at[v, :, part, :, cols])
        return to_dp(
            source, lambda k: gsr[v].at[k, :, :, cols],
            lambda k: gt_s.at[base, k], lambda k: gt_r.at[base, k], gather_kind[v],
        )

    pre_copies = {}
    back_copies = {}

    def pre_part(v):
        def body(j, carry):
            cols = pl.ds(pl.multiple_of(j * rtile, rtile), rtile)
            ps[v, :, cols] = dot_nt(gd[v], wi[v, cols, :]).astype(BF16)
            return carry

        lax.fori_loop(0, rank // rtile, body, 0)
        pre_copies[v] = to_tensor(
            ps.at[v], lambda k: pr.at[k, v], lambda k: pre_sem.at[0, v, k], lambda k: pre_sem.at[1, v, k]
        )
        for item in pre_copies[v]:
            item.start()

    def back_part(t, v):
        def body(j, carry):
            cols = pl.ds(pl.multiple_of(j * rtile, rtile), rtile)
            bs[v, t, :, cols] = dot_nt(ca[v, t], wo[v, cols, :]).astype(BF16)
            return carry

        lax.fori_loop(0, rank // rtile, body, 0)
        back_copies[t, v] = to_tensor(
            bs.at[v, t], lambda k: br.at[k, v, t],
            lambda k: back_sem.at[0, v * steps + t, k], lambda k: back_sem.at[1, v * steps + t, k],
        )
        for item in back_copies[t, v]:
            item.start()

    def finish_pre(v, which_steps):
        for t in which_steps:
            rows = pl.ds(t * tok, tok)
            total = ps[v, rows, :].astype(F32)
            for k in range(nt - 1):
                total = total + pr[k, v, rows, :].astype(F32)
            pre = inv_t[v, :, t:t + 1] * total
            sigma = jax.nn.sigmoid(pre)
            presum[v, rows, :] = total
            hid_t[v, :, rows] = jnp.transpose(pre * sigma).astype(BF16)
            slope[v, rows, :] = sigma * (1.0 + pre * (1.0 - sigma))

    def finish_back(t, v):
        for item in back_copies[t, v]:
            item.wait_recv()
        rows = pl.ds(t * tok, tok)
        inv = inv_t[v, :, t:t + 1]
        total = bs[v, t].astype(F32)
        for k in range(nt - 1):
            total = total + br[k, v, t].astype(F32)
        grad_pre = total * slope[v, rows, :]
        scaled = inv * grad_pre
        gs[v, rows, :] = scaled.astype(BF16)
        gs_t[v, :, :, :, rows] = jnp.transpose(scaled).astype(BF16).reshape(na, nb, rc, tok)
        for item in gs_copies(t, v):
            item.start()
        if t == steps - 1:
            for item in copies_one(0, v) + copies_one(1, v):
                item.start()
        radial = jnp.sum(grad_pre * presum[v, rows, :], axis=-1, keepdims=True)
        coef = inv * inv * inv * radial * (1.0 / full)

        def body(j, carry):
            cols = pl.ds(pl.multiple_of(j * tile, tile), tile)
            lifted = jnp.dot(gs[v, rows, :], wi[v, :, cols], preferred_element_type=F32)
            out = (
                ca[v, t, :, cols].astype(F32)
                + gn_ref[v, :, cols] * lifted
                - xs[t, v, :, cols].astype(F32) * coef
            ).astype(BF16)
            if t < steps - 1:
                ob[t, v, :, cols] = out
            else:
                lv[v, :, cols] = out
            return carry

        lax.fori_loop(0, wid // tile, body, 0)

    half_tok = tok // 2

    def pipe_copies(t, v, slot):
        parts = [(0, half_tok), (half_tok, half_tok)] if slot == 0 else [(0, tok)]
        return [
            pltpu.make_async_remote_copy(
                src_ref=ob.at[t, v, pl.ds(start, size)], dst_ref=ca.at[slot, t + 1, pl.ds(start, size)],
                send_sem=pipe_s.at[t, v, k], recv_sem=pipe_r.at[t, slot, k],
                device_id={"pipe": prev_p}, device_id_type=MESH,
            )
            for k, (start, size) in enumerate(parts)
        ]

    def send_on(t, v, first, last):
        @pl.when(me_p > 0)
        def _():
            for item in pipe_copies(t, v, v)[first:last]:
                item.start()

        if v == 1:
            @pl.when(me_p == 0)
            def _():
                for item in pipe_copies(t, 1, 0):
                    item.start()

    def sent_on(t, v):
        @pl.when(me_p > 0)
        def _():
            for item in pipe_copies(t, v, v):
                item.wait_send()

        if v == 1:
            @pl.when(me_p == 0)
            def _():
                for item in pipe_copies(t, 1, 0):
                    item.wait_send()

    def take(t, v):
        if v == 0:
            for item in pipe_copies(t - 1, v, v):
                item.wait_recv()
        else:
            @pl.when(me_p < npipe - 1)
            def _():
                for item in pipe_copies(t - 1, v, v):
                    item.wait_recv()

            @pl.when(me_p == npipe - 1)
            def _():
                stats = stl[...]
                for k in range(ndp - 1):
                    stats = stats + str_[k]
                means = stats[0:1] / jnp.maximum(stats[1:2], 1.0) + stats[2:3] * (1.0 / ndp)
                tok_row = lax.broadcasted_iota(jnp.int32, (tok, lanes), 0)
                tok_lane = lax.broadcasted_iota(jnp.int32, (tok, lanes), 1)
                hot = jnp.zeros((tok, lanes), F32)
                begin = 0
                for k in range(seq_count):
                    finish = begin + len_ref[t - 1, 0, k]
                    inside = (tok_row >= begin) & (tok_row < finish)
                    value = jnp.where(tok_lane == ids_ref[t - 1, 0, k], 1.0, 0.0)
                    value = value - jnp.where(tok_lane == unit_lane, rew_ref[t - 1, 0, k], 0.0)
                    hot = hot + jnp.where(inside, value, 0.0)
                    begin = finish
                weight = jnp.sum(hot * means, axis=-1, keepdims=True)
                ca[1, t] = (weight * lp[t - 1].astype(F32)).astype(BF16)

    def grad_out(v):
        def body(j, carry):
            for dest, off in ((gba, 0), (gbb, half)):
                cols = pl.ds(pl.multiple_of(j * tile, tile), tile)
                from_cols = pl.ds(pl.multiple_of(off + j * tile, tile), tile)
                right = ca[v, :, :, from_cols].reshape(steps * tok, tile)
                value = jnp.dot(hid_t[v], right, preferred_element_type=F32).astype(BF16)
                dest[v, :, :, :, cols] = value.reshape(na, nb, rc, tile)
            return carry

        lax.fori_loop(0, half // tile, body, 0)

    def grad_in(v):
        for item in gd_copies(v):
            item.wait_recv()
        for t in range(steps):
            for item in gs_copies(t, v):
                item.wait_recv()
        own = gs_t[v, me_h] if v == 0 else gs_t[v, :, me_l]
        width = nb if v == 0 else na
        own = own.reshape(width * rc, steps * tok)
        dest = p2i0 if v == 0 else p2i1

        def body(j, carry):
            cols = pl.ds(pl.multiple_of(j * tile, tile), tile)
            value = jnp.dot(own, gd[v, :, cols], preferred_element_type=F32)
            for k in range((na if v == 0 else nb) - 1):
                left = gsr[v][k].reshape(width * rc, steps * tok)
                value = value + jnp.dot(left, gdr[v][k, :, cols], preferred_element_type=F32)
            dest[:, :, cols] = value.astype(BF16).reshape(width, rc, tile)
            return carry

        lax.fori_loop(0, wid // tile, body, 0)
        for item in copies_two(2, v):
            item.start()

    def copies_one(which, v):
        base = which * vs + v
        if which == 0:
            return to_dp(
                lambda part: gba.at[v, :, part], lambda k: r1a.at[v, k],
                lambda k: r1_s.at[base, k], lambda k: r1_r.at[base, k], "l",
            )
        return to_dp(
            lambda part: gbb.at[v, part], lambda k: r1b.at[v, k],
            lambda k: r1_s.at[base, k], lambda k: r1_r.at[base, k], "h",
        )

    def copies_two(which, v):
        base = which * vs + v
        if which == 0:
            source, dest, kind = p2a.at[v], r2a.at[v], "h"
        elif which == 1:
            source, dest, kind = p2b.at[v], r2b.at[v], "l"
        elif v == 1:
            source, dest, kind = p2i1, r2i1, "h"
        else:
            source, dest, kind = p2i0, r2i0, "l"
        return to_dp(
            lambda part: source.at[part], lambda k: dest.at[k],
            lambda k: r2_s.at[base, k], lambda k: r2_r.at[base, k], kind,
        )

    def middle(which, v):
        for item in copies_one(which, v):
            item.wait_recv()
        if which == 0:
            total = gba[v, :, me_l].astype(F32)
            for k in range(nb - 1):
                total = total + r1a[v, k].astype(F32)
            p2a[v] = total.astype(BF16)
        else:
            total = gbb[v, me_h].astype(F32)
            for k in range(na - 1):
                total = total + r1b[v, k].astype(F32)
            p2b[v] = total.astype(BF16)
        for item in copies_two(which, v):
            item.start()

    scale = 1.0 / (ndp * tok)

    def final(which, v):
        for item in copies_two(which, v):
            item.wait_recv()
        along_h = which == 0 or (which == 2 and v == 1)
        source = {0: p2a.at[v], 1: p2b.at[v], 2: p2i1 if v == 1 else p2i0}[which]
        got = {0: r2a.at[v], 1: r2b.at[v], 2: r2i1 if v == 1 else r2i0}[which]
        total = source[me_h if along_h else me_l].astype(F32)
        for k in range((na if along_h else nb) - 1):
            total = total + got[k].astype(F32)
        if which == 2:
            fi[v] = total * scale
        else:
            fo[v, :, pl.ds(which * half, half)] = total * scale

    loads[0].wait()
    loads[1].wait()
    back_part(0, 1)
    loads[2].wait()
    prep(1)
    loads[3].wait()
    pre_part(1)
    loads[4].wait()
    prep(0)
    finish_sq(1)
    for item in pre_copies[1]:
        item.wait_recv()
    finish_pre(1, [0])
    finish_back(0, 1)
    send_on(0, 1, 0, 1)
    loads[5].wait()
    loads[6].wait()
    back_part(0, 0)
    loads[7].wait()
    pre_part(0)
    finish_pre(1, range(1, steps))
    finish_sq(0)
    for item in pre_copies[0]:
        item.wait_recv()
    finish_pre(0, [0])
    finish_back(0, 0)
    send_on(0, 0, 0, 1)
    finish_pre(0, range(1, steps))
    loads[8].wait()
    for item in stat_copies:
        item.wait_recv()
    for t in range(1, steps):
        for v in (1, 0):
            take(t, v)
            back_part(t, v)
            if t == steps - 1:
                grad_out(v)
            finish_back(t, v)
            if t < steps - 1:
                send_on(t, v, 0, 1)
                if v == 1:
                    send_on(t - 1, 0, 1, 2)
                elif t == steps - 2:
                    send_on(t, 0, 1, 2)
            elif v == 1:
                grad_in(1)
                middle(0, 1)
                middle(1, 1)
    grad_in(0)
    middle(0, 0)
    middle(1, 0)
    for v in (1, 0):
        for which in (2, 0, 1):
            final(which, v)
    for item in stat_copies + sq_copies(0) + sq_copies(1):
        item.wait_send()
    for v in range(vs):
        for item in pre_copies[v] + gd_copies(v):
            item.wait_send()
        for t in range(steps):
            for item in back_copies[t, v] + gs_copies(t, v):
                item.wait_send()
            if t < steps - 1:
                sent_on(t, v)
        for item in copies_one(0, v) + copies_one(1, v):
            item.wait_send()
        for which in range(3):
            for item in copies_two(which, v):
                item.wait_send()


def shards(
    saved_inputs, proj_in, proj_out, norm_gain, arriving, logp_grad, rewards, seq_lengths, group_ids
):
    nt = lax.axis_size("tensor")
    npipe = lax.axis_size("pipe")
    ndp = lax.axis_size("dp")
    steps, vs, _, tok, wid = saved_inputs.shape
    rank = proj_in.shape[2]
    new_count = logp_grad.shape[0]
    group_count = new_count * ndp * rewards.shape[2] // 8
    lanes = -(-(group_count + 1) // 128) * 128
    na, nb = factors(ndp)
    rc = rank // ndp
    half = wid // 2
    hm, lm = max(na - 1, 1), max(nb - 1, 1)
    dims = (steps, vs, tok, wid, rank, nt, npipe, ndp)
    peers = max(nt - 1, 1)
    any_spec = pl.BlockSpec(memory_space=pl.ANY)
    vmem = pl.BlockSpec(memory_space=pltpu.VMEM)
    V = pltpu.VMEM
    DMA = pltpu.SemaphoreType.DMA
    pmax = max(na, nb)
    smem = pl.BlockSpec(memory_space=pltpu.SMEM)
    scratch = [
        V((steps, vs, tok, wid), BF16),
        V((vs, steps * tok, wid), BF16),
        V((vs, steps, tok, wid), BF16),
        V((vs, rank, wid), BF16),
        V((vs, rank, wid), BF16),
        V((new_count, tok, wid), BF16),
        V((vs, steps * tok, rank), BF16),
        V((peers, vs, steps * tok, rank), BF16),
        V((vs, steps * tok, rank), F32),
        V((vs, steps * tok, rank), F32),
        V((vs, rank, steps * tok), BF16),
        V((vs, steps * tok, rank), BF16),
        V((vs, na, nb, rc, steps * tok), BF16),
        V((hm, nb, rc, steps * tok), BF16),
        V((lm, na, rc, steps * tok), BF16),
        V((hm, steps * tok, wid), BF16),
        V((lm, steps * tok, wid), BF16),
        V((vs, steps, tok, rank), BF16),
        V((peers, vs, steps, tok, rank), BF16),
        V((steps - 1, vs, tok, wid), BF16),
        V((vs, tok, 128), F32),
        V((peers, vs, tok, 128), F32),
        V((vs, tok, 128), F32),
        V((8, lanes), F32),
        V((max(ndp - 1, 1), 8, lanes), F32),
        V((vs, na, nb, rc, half), BF16),
        V((vs, na, nb, rc, half), BF16),
        V((vs, lm, na, rc, half), BF16),
        V((vs, hm, nb, rc, half), BF16),
        V((vs, na, rc, half), BF16),
        V((vs, nb, rc, half), BF16),
        V((vs, hm, rc, half), BF16),
        V((vs, lm, rc, half), BF16),
        V((nb, rc, wid), BF16),
        V((na, rc, wid), BF16),
        V((lm, rc, wid), BF16),
        V((hm, rc, wid), BF16),
        DMA((9,)),
        DMA((2, vs, peers)),
        DMA((2, max(ndp - 1, 1))),
        DMA((2, vs, peers)),
        DMA((2, vs * steps, peers)),
        DMA((steps - 1, vs, 2)),
        DMA((steps - 1, vs, 2)),
        DMA((vs, pmax)),
        DMA((vs, pmax)),
        DMA((vs * steps, pmax)),
        DMA((vs * steps, pmax)),
        DMA((2 * vs, pmax)),
        DMA((2 * vs, pmax)),
        DMA((3 * vs, pmax)),
        DMA((3 * vs, pmax)),
    ]
    grad_in, grad_out, leaving = pl.pallas_call(
        functools.partial(kernel, dims),
        out_shape=(
            V((vs, rc, wid), F32),
            V((vs, rc, wid), F32),
            V((vs, tok, wid), BF16),
        ),
        in_specs=[any_spec, any_spec, any_spec, vmem, any_spec, any_spec, smem, smem, smem],
        out_specs=(vmem, vmem, vmem),
        scratch_shapes=scratch,
        compiler_params=pltpu.CompilerParams(
            collective_id=0, has_side_effects=True, vmem_limit_bytes=56 * 1024 * 1024
        ),
    )(
        saved_inputs[:, :, 0], proj_in[:, 0], proj_out[:, 0], norm_gain, arriving[:, 0], logp_grad,
        rewards, seq_lengths, group_ids,
    )
    return grad_in[:, None], grad_out[:, None], leaving[:, None]


def solution(mesh):
    return jax.shard_map(
        shards,
        mesh=mesh,
        in_specs=(
            P(None, None, "pipe", "dp", "tensor"),
            P(None, "pipe", None, "tensor"),
            P(None, "pipe", None, "tensor"),
            P(None, "pipe", "tensor"),
            P(None, "pipe", "dp", "tensor"),
            P(None, "dp", "tensor"),
            P(None, "dp", None),
            P(None, "dp", None),
            P(None, "dp", None),
        ),
        out_specs=(
            P(None, "pipe", "dp", "tensor"),
            P(None, "pipe", "dp", "tensor"),
            P(None, "pipe", "dp", "tensor"),
        ),
        check_vma=False,
    )
```

```python
import functools

import jax
import jax.numpy as jnp
from jax import lax
from jax.experimental import pallas as pl
from jax.experimental.pallas import tpu as pltpu
from jax.sharding import PartitionSpec as P

EPS = 1e-05
MESH = pl.DeviceIdType.MESH
F32 = jnp.float32
BF16 = jnp.bfloat16


def dot_nt(a, b):
    return lax.dot_general(a, b, (((1,), (1,)), ((), ())), preferred_element_type=F32)


def factors(n):
    low = 1
    for k in range(1, n + 1):
        if n % k == 0 and k * k <= n:
            low = k
    return low, n // low


def kernel(
    dims,
    x_hbm, wi_hbm, wo_hbm, gn_ref, ar_hbm, lp_hbm, rew_ref, len_ref, ids_ref,
    fi, fo, lv,
    xs, gd, ca, wi, wo, lp, ps, pr, presum, slope, hid_t, gs, gs_t, gsr0, gsr1, gdr0, gdr1, bs, br, ob,
    sqs, sqr, inv_t, stl, str_, gba, gbb, r1a, r1b, p2a, p2b, r2a, r2b, p2i0, p2i1, r2i0, r2i1,
    in_sem, sq_sem, st_sem, pre_sem, back_sem, pipe_s, pipe_r, gd_s, gd_r, gt_s, gt_r,
    r1_s, r1_r, r2_s, r2_r,
):
    steps, vs, tok, wid, rank, nt, npipe, ndp = dims
    na, nb = factors(ndp)
    rc = rank // ndp
    full = wid * nt
    tile = min(512, wid // 2)
    rtile = min(512, rank)
    half = wid // 2
    lanes = stl.shape[1]
    new_count, _, seq_count = rew_ref.shape
    unit_lane = new_count * ndp * seq_count // 8
    me_t = lax.axis_index("tensor")
    me_p = lax.axis_index("pipe")
    me_d = lax.axis_index("dp")
    me_h = me_d // nb
    me_l = me_d % nb
    prev_p = lax.rem(me_p + npipe - 1, npipe)
    next_p = lax.rem(me_p + 1, npipe)

    def load(src, dst, k):
        return pltpu.make_async_copy(src, dst, in_sem.at[k])

    loads = [
        load(ar_hbm.at[1], ca.at[1, 0], 0),
        load(wo_hbm.at[1], wo.at[1], 1),
        load(x_hbm.at[:, 1], xs.at[:, 1], 2),
        load(wi_hbm.at[1], wi.at[1], 3),
        load(x_hbm.at[:, 0], xs.at[:, 0], 4),
        load(ar_hbm.at[0], ca.at[0, 0], 5),
        load(wo_hbm.at[0], wo.at[0], 6),
        load(wi_hbm.at[0], wi.at[0], 7),
        load(lp_hbm, lp, 8),
    ]
    for item in loads:
        item.start()

    lane8 = lax.broadcasted_iota(jnp.int32, (8, lanes), 1)
    row8 = lax.broadcasted_iota(jnp.int32, (8, lanes), 0)
    stats_own = jnp.where((row8 == 2) & (lane8 == unit_lane), 1.0, 0.0)
    for n in range(new_count):
        for k in range(seq_count):
            value = jnp.where(row8 == 0, rew_ref[n, 0, k], jnp.where(row8 == 1, 1.0, 0.0))
            stats_own = stats_own + jnp.where(lane8 == ids_ref[n, 0, k], value, 0.0)
    stl[...] = stats_own

    barrier = pltpu.get_barrier_semaphore()
    for k in range(1, nt):
        pl.semaphore_signal(barrier, inc=1, device_id={"tensor": lax.rem(me_t + k, nt)}, device_id_type=MESH)
    for k in range(1, ndp):
        pl.semaphore_signal(barrier, inc=1, device_id={"dp": lax.rem(me_d + k, ndp)}, device_id_type=MESH)
    for other in (prev_p, next_p):
        pl.semaphore_signal(barrier, inc=1, device_id={"pipe": other}, device_id_type=MESH)
    pl.semaphore_wait(barrier, nt - 1 + ndp - 1 + 2)

    def to_tensor(src, dst_of, send_of, recv_of):
        return [
            pltpu.make_async_remote_copy(
                src_ref=src, dst_ref=dst_of(k - 1), send_sem=send_of(k - 1), recv_sem=recv_of(k - 1),
                device_id={"tensor": lax.rem(me_t + k, nt)}, device_id_type=MESH,
            )
            for k in range(1, nt)
        ]

    def to_dp(src_of, dst_of, send_of, recv_of, kind):
        out = []
        count = {"all": ndp, "h": na, "l": nb}[kind]
        for k in range(1, count):
            if kind == "all":
                who = lax.rem(me_d + k, ndp)
                part = who
            elif kind == "h":
                part = lax.rem(me_h + k, na)
                who = part * nb + me_l
            else:
                part = lax.rem(me_l + k, nb)
                who = me_h * nb + part
            out.append(
                pltpu.make_async_remote_copy(
                    src_ref=src_of(part), dst_ref=dst_of(k - 1), send_sem=send_of(k - 1), recv_sem=recv_of(k - 1),
                    device_id={"dp": who}, device_id_type=MESH,
                )
            )
        return out

    stat_copies = to_dp(lambda part: stl, lambda k: str_.at[k], lambda k: st_sem.at[0, k], lambda k: st_sem.at[1, k], "all")
    for item in stat_copies:
        item.start()

    lane = lax.broadcasted_iota(jnp.int32, (tok, 128), 1)

    def sq_copies(v):
        return to_tensor(
            sqs.at[v], lambda k: sqr.at[k, v], lambda k: sq_sem.at[0, v, k], lambda k: sq_sem.at[1, v, k]
        )

    def prep(v):
        def body(t, squares_all):
            row = xs[t, v].astype(F32)
            gd[v, pl.ds(pl.multiple_of(t * tok, tok), tok), :] = (row * gn_ref[v]).astype(BF16)
            squares = jnp.sum(row * row, axis=-1, keepdims=True)
            return jnp.where(lane == t, squares, squares_all)

        sqs[v] = lax.fori_loop(0, steps, body, jnp.zeros((tok, 128), F32))
        for item in sq_copies(v) + gd_copies(v):
            item.start()

    def finish_sq(v):
        for item in sq_copies(v):
            item.wait_recv()
        total = sqs[v]
        for k in range(nt - 1):
            total = total + sqr[k, v]
        inv_t[v] = 1.0 / jnp.sqrt(total * (1.0 / full) + EPS)

    gather_kind = ("h", "l")
    gdr = (gdr0, gdr1)
    gsr = (gsr0, gsr1)

    def gd_copies(v):
        return to_dp(
            lambda part: gd.at[v], lambda k: gdr[v].at[k],
            lambda k: gd_s.at[v, k], lambda k: gd_r.at[v, k], gather_kind[v],
        )

    def gs_copies(t, v):
        cols = pl.ds(t * tok, tok)
        base = v * steps + t
        source = (lambda part: gs_t.at[v, part, :, :, cols]) if v == 0 else (lambda part: gs_t.at[v, :, part, :, cols])
        return to_dp(
            source, lambda k: gsr[v].at[k, :, :, cols],
            lambda k: gt_s.at[base, k], lambda k: gt_r.at[base, k], gather_kind[v],
        )

    pre_copies = {}
    back_copies = {}

    def pre_part(v):
        def body(j, carry):
            cols = pl.ds(pl.multiple_of(j * rtile, rtile), rtile)
            ps[v, :, cols] = dot_nt(gd[v], wi[v, cols, :]).astype(BF16)
            return carry

        lax.fori_loop(0, rank // rtile, body, 0)
        pre_copies[v] = to_tensor(
            ps.at[v], lambda k: pr.at[k, v], lambda k: pre_sem.at[0, v, k], lambda k: pre_sem.at[1, v, k]
        )
        for item in pre_copies[v]:
            item.start()

    def back_part(t, v):
        def body(j, carry):
            cols = pl.ds(pl.multiple_of(j * rtile, rtile), rtile)
            bs[v, t, :, cols] = dot_nt(ca[v, t], wo[v, cols, :]).astype(BF16)
            return carry

        lax.fori_loop(0, rank // rtile, body, 0)
        back_copies[t, v] = to_tensor(
            bs.at[v, t], lambda k: br.at[k, v, t],
            lambda k: back_sem.at[0, v * steps + t, k], lambda k: back_sem.at[1, v * steps + t, k],
        )
        for item in back_copies[t, v]:
            item.start()

    def finish_pre(v, which_steps):
        for t in which_steps:
            rows = pl.ds(t * tok, tok)
            total = ps[v, rows, :].astype(F32)
            for k in range(nt - 1):
                total = total + pr[k, v, rows, :].astype(F32)
            pre = inv_t[v, :, t:t + 1] * total
            sigma = jax.nn.sigmoid(pre)
            presum[v, rows, :] = total
            hid_t[v, :, rows] = jnp.transpose(pre * sigma).astype(BF16)
            slope[v, rows, :] = sigma * (1.0 + pre * (1.0 - sigma))

    def finish_back(t, v):
        for item in back_copies[t, v]:
            item.wait_recv()
        rows = pl.ds(t * tok, tok)
        inv = inv_t[v, :, t:t + 1]
        total = bs[v, t].astype(F32)
        for k in range(nt - 1):
            total = total + br[k, v, t].astype(F32)
        grad_pre = total * slope[v, rows, :]
        scaled = inv * grad_pre
        gs[v, rows, :] = scaled.astype(BF16)
        gs_t[v, :, :, :, rows] = jnp.transpose(scaled).astype(BF16).reshape(na, nb, rc, tok)
        for item in gs_copies(t, v):
            item.start()
        if t == steps - 1:
            for item in copies_one(0, v) + copies_one(1, v):
                item.start()
        radial = jnp.sum(grad_pre * presum[v, rows, :], axis=-1, keepdims=True)
        coef = inv * inv * inv * radial * (1.0 / full)

        def body(j, carry):
            cols = pl.ds(pl.multiple_of(j * tile, tile), tile)
            lifted = jnp.dot(gs[v, rows, :], wi[v, :, cols], preferred_element_type=F32)
            out = (
                ca[v, t, :, cols].astype(F32)
                + gn_ref[v, :, cols] * lifted
                - xs[t, v, :, cols].astype(F32) * coef
            ).astype(BF16)
            if t < steps - 1:
                ob[t, v, :, cols] = out
            else:
                lv[v, :, cols] = out
            return carry

        lax.fori_loop(0, wid // tile, body, 0)

    half_tok = tok // 2

    def pipe_copies(t, v, slot):
        parts = [(0, half_tok), (half_tok, half_tok)] if slot == 0 else [(0, tok)]
        return [
            pltpu.make_async_remote_copy(
                src_ref=ob.at[t, v, pl.ds(start, size)], dst_ref=ca.at[slot, t + 1, pl.ds(start, size)],
                send_sem=pipe_s.at[t, v, k], recv_sem=pipe_r.at[t, slot, k],
                device_id={"pipe": prev_p}, device_id_type=MESH,
            )
            for k, (start, size) in enumerate(parts)
        ]

    def send_on(t, v, first, last):
        @pl.when(me_p > 0)
        def _():
            for item in pipe_copies(t, v, v)[first:last]:
                item.start()

        if v == 1:
            @pl.when(me_p == 0)
            def _():
                for item in pipe_copies(t, 1, 0):
                    item.start()

    def sent_on(t, v):
        @pl.when(me_p > 0)
        def _():
            for item in pipe_copies(t, v, v):
                item.wait_send()

        if v == 1:
            @pl.when(me_p == 0)
            def _():
                for item in pipe_copies(t, 1, 0):
                    item.wait_send()

    def take(t, v):
        if v == 0:
            for item in pipe_copies(t - 1, v, v):
                item.wait_recv()
        else:
            @pl.when(me_p < npipe - 1)
            def _():
                for item in pipe_copies(t - 1, v, v):
                    item.wait_recv()

            @pl.when(me_p == npipe - 1)
            def _():
                stats = stl[...]
                for k in range(ndp - 1):
                    stats = stats + str_[k]
                means = stats[0:1] / jnp.maximum(stats[1:2], 1.0) + stats[2:3] * (1.0 / ndp)
                tok_row = lax.broadcasted_iota(jnp.int32, (tok, lanes), 0)
                tok_lane = lax.broadcasted_iota(jnp.int32, (tok, lanes), 1)
                hot = jnp.zeros((tok, lanes), F32)
                begin = 0
                for k in range(seq_count):
                    finish = begin + len_ref[t - 1, 0, k]
                    inside = (tok_row >= begin) & (tok_row < finish)
                    value = jnp.where(tok_lane == ids_ref[t - 1, 0, k], 1.0, 0.0)
                    value = value - jnp.where(tok_lane == unit_lane, rew_ref[t - 1, 0, k], 0.0)
                    hot = hot + jnp.where(inside, value, 0.0)
                    begin = finish
                weight = jnp.sum(hot * means, axis=-1, keepdims=True)
                ca[1, t] = (weight * lp[t - 1].astype(F32)).astype(BF16)

    def grad_out(v):
        def body(j, carry):
            for dest, off in ((gba, 0), (gbb, half)):
                cols = pl.ds(pl.multiple_of(j * tile, tile), tile)
                from_cols = pl.ds(pl.multiple_of(off + j * tile, tile), tile)
                right = ca[v, :, :, from_cols].reshape(steps * tok, tile)
                value = jnp.dot(hid_t[v], right, preferred_element_type=F32).astype(BF16)
                dest[v, :, :, :, cols] = value.reshape(na, nb, rc, tile)
            return carry

        lax.fori_loop(0, half // tile, body, 0)

    def grad_in(v):
        for item in gd_copies(v):
            item.wait_recv()
        for t in range(steps):
            for item in gs_copies(t, v):
                item.wait_recv()
        own = gs_t[v, me_h] if v == 0 else gs_t[v, :, me_l]
        width = nb if v == 0 else na
        own = own.reshape(width * rc, steps * tok)
        dest = p2i0 if v == 0 else p2i1

        def body(j, carry):
            cols = pl.ds(pl.multiple_of(j * tile, tile), tile)
            value = jnp.dot(own, gd[v, :, cols], preferred_element_type=F32)
            for k in range((na if v == 0 else nb) - 1):
                left = gsr[v][k].reshape(width * rc, steps * tok)
                value = value + jnp.dot(left, gdr[v][k, :, cols], preferred_element_type=F32)
            dest[:, :, cols] = value.astype(BF16).reshape(width, rc, tile)
            return carry

        lax.fori_loop(0, wid // tile, body, 0)
        for item in copies_two(2, v):
            item.start()

    def copies_one(which, v):
        base = which * vs + v
        if which == 0:
            return to_dp(
                lambda part: gba.at[v, :, part], lambda k: r1a.at[v, k],
                lambda k: r1_s.at[base, k], lambda k: r1_r.at[base, k], "l",
            )
        return to_dp(
            lambda part: gbb.at[v, part], lambda k: r1b.at[v, k],
            lambda k: r1_s.at[base, k], lambda k: r1_r.at[base, k], "h",
        )

    def copies_two(which, v):
        base = which * vs + v
        if which == 0:
            source, dest, kind = p2a.at[v], r2a.at[v], "h"
        elif which == 1:
            source, dest, kind = p2b.at[v], r2b.at[v], "l"
        elif v == 1:
            source, dest, kind = p2i1, r2i1, "h"
        else:
            source, dest, kind = p2i0, r2i0, "l"
        return to_dp(
            lambda part: source.at[part], lambda k: dest.at[k],
            lambda k: r2_s.at[base, k], lambda k: r2_r.at[base, k], kind,
        )

    def middle(which, v):
        for item in copies_one(which, v):
            item.wait_recv()
        if which == 0:
            total = gba[v, :, me_l].astype(F32)
            for k in range(nb - 1):
                total = total + r1a[v, k].astype(F32)
            p2a[v] = total.astype(BF16)
        else:
            total = gbb[v, me_h].astype(F32)
            for k in range(na - 1):
                total = total + r1b[v, k].astype(F32)
            p2b[v] = total.astype(BF16)
        for item in copies_two(which, v):
            item.start()

    scale = 1.0 / (ndp * tok)

    def final(which, v):
        for item in copies_two(which, v):
            item.wait_recv()
        along_h = which == 0 or (which == 2 and v == 1)
        source = {0: p2a.at[v], 1: p2b.at[v], 2: p2i1 if v == 1 else p2i0}[which]
        got = {0: r2a.at[v], 1: r2b.at[v], 2: r2i1 if v == 1 else r2i0}[which]
        total = source[me_h if along_h else me_l].astype(F32)
        for k in range((na if along_h else nb) - 1):
            total = total + got[k].astype(F32)
        if which == 2:
            fi[v] = total * scale
        else:
            fo[v, :, pl.ds(which * half, half)] = total * scale

    loads[0].wait()
    loads[1].wait()
    back_part(0, 1)
    loads[2].wait()
    prep(1)
    loads[3].wait()
    pre_part(1)
    loads[4].wait()
    prep(0)
    finish_sq(1)
    for item in pre_copies[1]:
        item.wait_recv()
    finish_pre(1, [0])
    finish_back(0, 1)
    send_on(0, 1, 0, 2)
    loads[5].wait()
    loads[6].wait()
    back_part(0, 0)
    loads[7].wait()
    pre_part(0)
    finish_pre(1, range(1, steps))
    finish_sq(0)
    for item in pre_copies[0]:
        item.wait_recv()
    finish_pre(0, [0])
    finish_back(0, 0)
    send_on(0, 0, 0, 2)
    finish_pre(0, range(1, steps))
    loads[8].wait()
    for item in stat_copies:
        item.wait_recv()
    for t in range(1, steps):
        for v in (1, 0):
            take(t, v)
            back_part(t, v)
            if t == steps - 1:
                grad_out(v)
            finish_back(t, v)
            if t < steps - 1:
                send_on(t, v, 0, 2)
            elif v == 1:
                grad_in(1)
    middle(0, 1)
    middle(1, 1)
    grad_in(0)
    middle(0, 0)
    middle(1, 0)
    for v in (1, 0):
        for which in (2, 0, 1):
            final(which, v)
    for item in stat_copies + sq_copies(0) + sq_copies(1):
        item.wait_send()
    for v in range(vs):
        for item in pre_copies[v] + gd_copies(v):
            item.wait_send()
        for t in range(steps):
            for item in back_copies[t, v] + gs_copies(t, v):
                item.wait_send()
            if t < steps - 1:
                sent_on(t, v)
        for item in copies_one(0, v) + copies_one(1, v):
            item.wait_send()
        for which in range(3):
            for item in copies_two(which, v):
                item.wait_send()


def shards(
    saved_inputs, proj_in, proj_out, norm_gain, arriving, logp_grad, rewards, seq_lengths, group_ids
):
    nt = lax.axis_size("tensor")
    npipe = lax.axis_size("pipe")
    ndp = lax.axis_size("dp")
    steps, vs, _, tok, wid = saved_inputs.shape
    rank = proj_in.shape[2]
    new_count = logp_grad.shape[0]
    group_count = new_count * ndp * rewards.shape[2] // 8
    lanes = -(-(group_count + 1) // 128) * 128
    na, nb = factors(ndp)
    rc = rank // ndp
    half = wid // 2
    hm, lm = max(na - 1, 1), max(nb - 1, 1)
    dims = (steps, vs, tok, wid, rank, nt, npipe, ndp)
    peers = max(nt - 1, 1)
    any_spec = pl.BlockSpec(memory_space=pl.ANY)
    vmem = pl.BlockSpec(memory_space=pltpu.VMEM)
    V = pltpu.VMEM
    DMA = pltpu.SemaphoreType.DMA
    pmax = max(na, nb)
    smem = pl.BlockSpec(memory_space=pltpu.SMEM)
    scratch = [
        V((steps, vs, tok, wid), BF16),
        V((vs, steps * tok, wid), BF16),
        V((vs, steps, tok, wid), BF16),
        V((vs, rank, wid), BF16),
        V((vs, rank, wid), BF16),
        V((new_count, tok, wid), BF16),
        V((vs, steps * tok, rank), BF16),
        V((peers, vs, steps * tok, rank), BF16),
        V((vs, steps * tok, rank), F32),
        V((vs, steps * tok, rank), F32),
        V((vs, rank, steps * tok), BF16),
        V((vs, steps * tok, rank), BF16),
        V((vs, na, nb, rc, steps * tok), BF16),
        V((hm, nb, rc, steps * tok), BF16),
        V((lm, na, rc, steps * tok), BF16),
        V((hm, steps * tok, wid), BF16),
        V((lm, steps * tok, wid), BF16),
        V((vs, steps, tok, rank), BF16),
        V((peers, vs, steps, tok, rank), BF16),
        V((steps - 1, vs, tok, wid), BF16),
        V((vs, tok, 128), F32),
        V((peers, vs, tok, 128), F32),
        V((vs, tok, 128), F32),
        V((8, lanes), F32),
        V((max(ndp - 1, 1), 8, lanes), F32),
        V((vs, na, nb, rc, half), BF16),
        V((vs, na, nb, rc, half), BF16),
        V((vs, lm, na, rc, half), BF16),
        V((vs, hm, nb, rc, half), BF16),
        V((vs, na, rc, half), BF16),
        V((vs, nb, rc, half), BF16),
        V((vs, hm, rc, half), BF16),
        V((vs, lm, rc, half), BF16),
        V((nb, rc, wid), BF16),
        V((na, rc, wid), BF16),
        V((lm, rc, wid), BF16),
        V((hm, rc, wid), BF16),
        DMA((9,)),
        DMA((2, vs, peers)),
        DMA((2, max(ndp - 1, 1))),
        DMA((2, vs, peers)),
        DMA((2, vs * steps, peers)),
        DMA((steps - 1, vs, 2)),
        DMA((steps - 1, vs, 2)),
        DMA((vs, pmax)),
        DMA((vs, pmax)),
        DMA((vs * steps, pmax)),
        DMA((vs * steps, pmax)),
        DMA((2 * vs, pmax)),
        DMA((2 * vs, pmax)),
        DMA((3 * vs, pmax)),
        DMA((3 * vs, pmax)),
    ]
    grad_in, grad_out, leaving = pl.pallas_call(
        functools.partial(kernel, dims),
        out_shape=(
            V((vs, rc, wid), F32),
            V((vs, rc, wid), F32),
            V((vs, tok, wid), BF16),
        ),
        in_specs=[any_spec, any_spec, any_spec, vmem, any_spec, any_spec, smem, smem, smem],
        out_specs=(vmem, vmem, vmem),
        scratch_shapes=scratch,
        compiler_params=pltpu.CompilerParams(
            collective_id=0, has_side_effects=True, vmem_limit_bytes=56 * 1024 * 1024
        ),
    )(
        saved_inputs[:, :, 0], proj_in[:, 0], proj_out[:, 0], norm_gain, arriving[:, 0], logp_grad,
        rewards, seq_lengths, group_ids,
    )
    return grad_in[:, None], grad_out[:, None], leaving[:, None]


def solution(mesh):
    return jax.shard_map(
        shards,
        mesh=mesh,
        in_specs=(
            P(None, None, "pipe", "dp", "tensor"),
            P(None, "pipe", None, "tensor"),
            P(None, "pipe", None, "tensor"),
            P(None, "pipe", "tensor"),
            P(None, "pipe", "dp", "tensor"),
            P(None, "dp", "tensor"),
            P(None, "dp", None),
            P(None, "dp", None),
            P(None, "dp", None),
        ),
        out_specs=(
            P(None, "pipe", "dp", "tensor"),
            P(None, "pipe", "dp", "tensor"),
            P(None, "pipe", "dp", "tensor"),
        ),
        check_vma=False,
    )
```
